32 devices in a mesh: ka: 4 (over y, x), pb: 8 (over z, core).
Axes of the slice: x: 2, y: 2, z: 4, core: 2. Of those that a mesh axis runs over, the one named last changes fastest.
Arguments:
- bloch_elements: float32 [2, 96, 96, 64, 64], P(None, 'ka', 'pb'), may hold values from -768 to 768
- gauge: float32 [2, 96, 64, 64], P(None, 'ka'), may hold values from -0.5 to 0.5
- kq_index: int32 [96, 96], P('ka', 'pb'), may hold values from 0 to 95, as said below
- qpoint: int32 [96], replicated, may hold values from 0 to 95, as said below
- re_vectors: int32 [128, 3], replicated, may hold values from -3 to 3
- re_weight: int32 [128], replicated, may hold values from 1 to 4
- rp_vectors: int32 [128, 3], replicated, may hold values from -3 to 3
- rp_weight: int32 [128], replicated, may hold values from 1 to 4
Outputs:
- wannier_elements: float32 [2, 128, 128, 64, 64], P(None, 'ka', 'pb')
The draws below stay inside these ranges and needn't reach their ends.
Inputs may be any that keep to these rules, and one draw needn't show every extreme that they name: `qpoint`: each mesh index appears in exactly one slot. kq_index[k, s] is the mesh index of point k plus the point of slot s, folded back into the mesh.
All inputs are finite; a program needn't handle non-finite values.
Results may differ from the reference program's by a relative error of at most 0.000071.
Values sent between devices are 32-bit elements; how exact they have to be, the bound alone decides.
A program may use at most 192 MiB of HBM per device.

```python
import math
import jax
import jax.numpy as jnp
from jax import lax

NB = 64
MK1 = 4
MK2 = 6
MK3 = 4
NRE = 128
NRP = 128
NK = 96
NQ = 96


def mesh_order(key):
    return jax.random.permutation(jax.random.fold_in(key, 17), NQ).astype(jnp.int32)


def draw_qpoint(key, part):
    return mesh_order(key)


def draw_kq_index(key, part):
    qpoint = mesh_order(key)
    points = jnp.arange(NK, dtype=jnp.int32)
    first_sum = (points[:, None] // (MK2 * MK3) + qpoint[None, :] // (MK2 * MK3)) % MK1
    second_sum = (points[:, None] // MK3 % MK2 + qpoint[None, :] // MK3 % MK2) % MK2
    third_sum = (points[:, None] % MK3 + qpoint[None, :] % MK3) % MK3
    return ((first_sum * MK2 + second_sum) * MK3 + third_sum).astype(jnp.int32)


def place_ends(drawn, own_key, least, high):
    longest = drawn.shape.index(max(drawn.shape))
    spots = []
    for shift in (0, 1):
        where = [jax.random.randint(jax.random.fold_in(own_key, axis), (), 0, length) for axis, length in enumerate(drawn.shape)]
        where[longest] = (where[longest] + shift) % drawn.shape[longest]
        spots.append(tuple(where))
    return drawn.at[spots[0]].set(least).at[spots[1]].set(high)


def shard_levels(own_key, dims, shards, least, largest):
    level = 1.0
    for dim, blocks in shards:
        steps = jax.random.uniform(jax.random.fold_in(jax.random.fold_in(own_key, 6), dim), (blocks,), jnp.float32, least / len(shards), largest / len(shards))
        level = level * jnp.repeat(jnp.exp(steps), dims[dim] // blocks).reshape((-1,) + (1,) * (len(dims) - 1 - dim))
    return level


def bell_draw(stream_key, extent, spread, limit, split=(), kind=jnp.bfloat16):
    drawn = spread * jax.random.normal(stream_key, extent, jnp.float32)
    if split:
        drawn = drawn * shard_levels(stream_key, extent, split, -0.22, 0.18)
    return jnp.clip(drawn, -limit, limit).astype(kind)


def setup_inputs(seed: int = 0) -> dict:
    arg_keys = jax.random.split(jax.random.key(seed), 9)
    return {
        "bloch_elements": bell_draw(arg_keys[0], (2, NK, NQ, NB, NB), 128.0, 768.0, ((1, 4), (2, 8)), jnp.float32),
        "gauge": bell_draw(arg_keys[1], (2, NK, NB, NB), (2 * NB) ** -0.5, 0.5, ((1, 4),), jnp.float32),
        "kq_index": draw_kq_index(jax.random.fold_in(arg_keys[8], 71), 0),
        "qpoint": draw_qpoint(jax.random.fold_in(arg_keys[8], 71), 0),
        "re_vectors": place_ends(jax.random.randint(arg_keys[4], (NRE, 3), -3, 4), jax.random.fold_in(arg_keys[4], 1), -3, 3).astype(jnp.int32),
        "re_weight": place_ends(jax.random.randint(arg_keys[5], (NRE,), 1, 5), jax.random.fold_in(arg_keys[5], 1), 1, 4).astype(jnp.int32),
        "rp_vectors": place_ends(jax.random.randint(arg_keys[6], (NRP, 3), -3, 4), jax.random.fold_in(arg_keys[6], 1), -3, 3).astype(jnp.int32),
        "rp_weight": place_ends(jax.random.randint(arg_keys[7], (NRP,), 1, 5), jax.random.fold_in(arg_keys[7], 1), 1, 4).astype(jnp.int32),
    }


def mesh_phase(vectors, points, total_count):
    first_index = points // (MK2 * MK3)
    second_index = (points // MK3) % MK2
    third_index = points % MK3
    phase_turns = (vectors[:, 0:1] * (first_index * (MK2 * MK3))[None, :]
                   + vectors[:, 1:2] * (second_index * (MK1 * MK3))[None, :]
                   + vectors[:, 2:3] * (third_index * (MK1 * MK2))[None, :])
    phase_turns = jnp.mod(phase_turns, MK1 * MK2 * MK3)
    angles = phase_turns.astype(jnp.float32) * (2.0 * math.pi / (MK1 * MK2 * MK3))
    return jnp.cos(angles) / total_count, jnp.sin(angles) / total_count


def rotate_gauge(elements, left_side, right_side):
    exact_mode = lax.Precision.HIGHEST
    real_part = jnp.matmul(elements[0], right_side[0], precision=exact_mode) - jnp.matmul(elements[1], right_side[1], precision=exact_mode)
    imag_part = jnp.matmul(elements[0], right_side[1], precision=exact_mode) + jnp.matmul(elements[1], right_side[0], precision=exact_mode)
    left_real = jnp.swapaxes(left_side[0], -1, -2)
    left_imag = jnp.swapaxes(left_side[1], -1, -2)
    rot_real = jnp.matmul(left_real, real_part, precision=exact_mode) + jnp.matmul(left_imag, imag_part, precision=exact_mode)
    rot_imag = jnp.matmul(left_real, imag_part, precision=exact_mode) - jnp.matmul(left_imag, real_part, precision=exact_mode)
    return jnp.stack([rot_real, rot_imag])


def lattice_sum(table, planes, form):
    exact_mode = lax.Precision.HIGHEST
    cosine, sine_table = table
    real_part = jnp.einsum(form, cosine, planes[0], precision=exact_mode) + jnp.einsum(form, sine_table, planes[1], precision=exact_mode)
    imag_part = jnp.einsum(form, cosine, planes[1], precision=exact_mode) - jnp.einsum(form, sine_table, planes[0], precision=exact_mode)
    return jnp.stack([real_part, imag_part])


def reference(bloch_elements, gauge, kq_index, qpoint, re_vectors, re_weight, rp_vectors, rp_weight):
    def one_point(point_index):
        elements = lax.dynamic_index_in_dim(bloch_elements, point_index, 1, keepdims=False)
        targets = lax.dynamic_index_in_dim(kq_index, point_index, 0, keepdims=False)
        left_side = jnp.take(gauge, targets, axis=1)
        right_side = lax.dynamic_index_in_dim(gauge, point_index, 1, keepdims=False)
        return rotate_gauge(elements, left_side, right_side)

    rotated = lax.map(one_point, jnp.arange(NK, dtype=jnp.int32))
    block_width = NB * NB // 16
    blocks = rotated.reshape(NK, 2, NQ, 16, block_width).transpose(3, 1, 0, 2, 4)
    k_table = mesh_phase(re_vectors, jnp.arange(NK, dtype=jnp.int32), NK)
    q_table = mesh_phase(rp_vectors, qpoint, NQ)

    def both_sums(block):
        electron = lattice_sum(k_table, block, "rk,kqc->rqc")
        return lattice_sum(q_table, electron, "pq,rqc->rpc")

    summed = lax.map(both_sums, blocks)
    summed = summed.transpose(1, 2, 3, 0, 4).reshape(2, NRE, NRP, NB, NB)
    weight = (re_weight[:, None] * rp_weight[None, :]).astype(jnp.float32)
    return summed / weight[None, :, :, None, None]
```

```python
import functools
import math

import jax
import jax.numpy as jnp
from jax import lax
from jax.experimental import pallas as pl
from jax.experimental.pallas import tpu as pltpu
from jax.sharding import PartitionSpec as P

MK1 = 4
MK2 = 6
MK3 = 4
LANES = 128
VMEM_BYTES = 67_000_000
MESH = pl.DeviceIdType.MESH


def mesh_phase(vectors, points, total_count):
    first_index = points // (MK2 * MK3)
    second_index = points // MK3 % MK2
    third_index = points % MK3
    phase_turns = (
        vectors[:, 0:1] * (first_index * (MK2 * MK3))[None, :]
        + vectors[:, 1:2] * (second_index * (MK1 * MK3))[None, :]
        + vectors[:, 2:3] * (third_index * (MK1 * MK2))[None, :]
    )
    phase_turns = jnp.mod(phase_turns, MK1 * MK2 * MK3)
    angles = phase_turns.astype(jnp.float32) * (2.0 * math.pi / (MK1 * MK2 * MK3))
    return (jnp.cos(angles) / total_count, jnp.sin(angles) / total_count)


def rotate_gauge(elements, left_side, right_side):
    exact_mode = lax.Precision.HIGH
    real_part = jnp.matmul(elements[0], right_side[0], precision=exact_mode) - jnp.matmul(
        elements[1], right_side[1], precision=exact_mode
    )
    imag_part = jnp.matmul(elements[0], right_side[1], precision=exact_mode) + jnp.matmul(
        elements[1], right_side[0], precision=exact_mode
    )
    left_real = jnp.swapaxes(left_side[0], -1, -2)
    left_imag = jnp.swapaxes(left_side[1], -1, -2)
    rot_real = jnp.matmul(left_real, real_part, precision=exact_mode) + jnp.matmul(
        left_imag, imag_part, precision=exact_mode
    )
    rot_imag = jnp.matmul(left_real, imag_part, precision=exact_mode) - jnp.matmul(
        left_imag, real_part, precision=exact_mode
    )
    return jnp.stack([rot_real, rot_imag])


def complex_table(table, count):
    cosine, sine_table = table
    real_rows = jnp.stack([cosine, sine_table], axis=1)
    imag_rows = jnp.stack([-sine_table, cosine], axis=1)
    scale = count.astype(jnp.float32)[None, :, None, None]
    return jnp.stack([real_rows, imag_rows]) / scale


def local_general(bloch_elements, gauge, kq_index, qpoint, re_vectors, re_weight, rp_vectors, rp_weight):
    local_k = bloch_elements.shape[1]
    local_q = bloch_elements.shape[2]
    bands = bloch_elements.shape[3]
    pairs = bands * bands
    gathered = lax.all_gather(gauge, "ka", axis=1, tiled=True)
    left_side = jnp.take(gathered, kq_index, axis=1)
    rotated = rotate_gauge(bloch_elements, left_side, gauge[:, :, None])
    rotated = rotated.reshape(2, local_k, local_q, pairs)
    k_count = gathered.shape[1]
    q_count = qpoint.shape[0]
    k_table = mesh_phase(re_vectors, jnp.arange(k_count, dtype=jnp.int32), k_count)
    q_table = mesh_phase(rp_vectors, qpoint, q_count)
    ka_count = lax.axis_size("ka")
    pb_count = lax.axis_size("pb")
    re_local = re_vectors.shape[0] // ka_count
    rp_local = rp_vectors.shape[0] // pb_count
    devices = ka_count * pb_count
    column_width = pairs // devices
    leaving = rotated.reshape(2, local_k, local_q, devices, column_width).transpose(3, 0, 1, 2, 4)
    leaving = leaving.reshape(devices, 2 * local_k * local_q, column_width)
    joined = lax.all_to_all(leaving, ("ka", "pb"), split_axis=0, concat_axis=0, tiled=True)
    joined = joined.reshape(ka_count, pb_count, 2, local_k, local_q, column_width)
    k_blocks = complex_table(k_table, re_weight).reshape(
        2, ka_count, re_local, 2, ka_count, local_k
    )
    q_blocks = complex_table(q_table, rp_weight).reshape(
        2, pb_count, rp_local, 2, pb_count, local_q
    )
    exact_mode = lax.Precision.HIGH
    electron = jnp.einsum("dauemk,mpeklx->dauplx", k_blocks, joined, precision=exact_mode)
    spread = jnp.einsum("fbvdpl,dauplx->abfuvx", q_blocks, electron, precision=exact_mode)
    spread = spread.reshape(devices, 2 * re_local * rp_local, column_width)
    result = lax.all_to_all(spread, ("ka", "pb"), split_axis=0, concat_axis=0, tiled=True)
    result = result.reshape(devices, 2, re_local, rp_local, column_width)
    return result.transpose(1, 2, 3, 0, 4).reshape(2, re_local, rp_local, bands, bands)


def split(x):
    high = x.astype(jnp.bfloat16)
    low = (x - high.astype(jnp.float32)).astype(jnp.bfloat16)
    return high, low


def dot(a, b):
    return jnp.dot(a, b, preferred_element_type=jnp.float32)


def swap(x, sign):
    return pltpu.roll(x, x.shape[-1] // 2, x.ndim - 1) * sign


class Plan:
    def __init__(self, ka, pb, local_k, local_q, bands, re_count, rp_count):
        self.ka, self.pb = ka, pb
        self.devices = ka * pb
        self.local_k, self.local_q, self.bands = local_k, local_q, bands
        self.k_count, self.q_count = ka * local_k, pb * local_q
        self.re_count, self.rp_count = re_count, rp_count
        self.re_local, self.rp_local = re_count // ka, rp_count // pb
        self.fits = (
            2 * bands == LANES
            and bands % self.devices == 0
            and pb % 2 == 0
            and ka % 2 == 0
            and local_k % 6 == 0
        )
        if not self.fits:
            return
        self.rows = bands // self.devices
        self.share = self.rows * local_q
        self.kc = 3
        self.k_chunks = local_k // self.kc
        self.rpc = 2
        self.rp_chunks = self.rp_local // self.rpc
        self.width = self.rows * pb
        self.piece = self.rpc * self.rows * self.k_count
        self.block = self.re_local * self.rpc * self.width
        self.slots = 2
        self.fits = (
            self.share % 8 == 0
            and self.k_count % 16 == 0
            and (pb * self.share) % 16 == 0
            and self.width % 8 == 0
            and self.rp_local % self.rpc == 0
            and self.rp_chunks > self.slots
        )


def kernel(
    p,
    bloch,
    v_in,
    right,
    kq,
    tq,
    tk,
    out,
    gbuf,
    vg,
    rot,
    x_buf,
    y_buf,
    z_buf,
    w_buf,
    g_sem,
    own_sem,
    vs_sem,
    v1_sem,
    f_sem,
    v2_sem,
    s1_sem,
    r1_sem,
    s2_sem,
    r2_sem,
    s3_sem,
    r3_sem,
):
    a = lax.axis_index("ka")
    b = lax.axis_index("pb")
    me = a * p.pb + b
    core = b % 2
    sibling = b + 1 - 2 * core
    half = p.local_k // 2
    lane = lax.broadcasted_iota(jnp.int32, (1, LANES), 1)
    sign = jnp.where(lane < p.bands, 1.0, -1.0).astype(jnp.float32)

    def load_g(k):
        return pltpu.make_async_copy(bloch.at[:, k], gbuf.at[k % 2], g_sem.at[k % 2])

    load_g(0).start()
    own_v = pltpu.make_async_copy(v_in, vg.at[pl.ds(a * p.local_k, p.local_k)], own_sem)
    own_v.start()

    barrier = pltpu.get_barrier_semaphore()

    @pl.loop(1, p.devices)
    def _(o):
        t = (me + o) % p.devices
        pl.semaphore_signal(barrier, inc=1, device_id=(t // p.pb, t % p.pb), device_id_type=MESH)

    pl.semaphore_wait(barrier, p.devices - 1)

    def send_v(i):
        return pltpu.make_async_remote_copy(
            src_ref=v_in.at[pl.ds(core * half, half)],
            dst_ref=vg.at[pl.ds(a * p.local_k + core * half, half)],
            send_sem=vs_sem.at[i],
            recv_sem=v1_sem.at[i],
            device_id=((a + i) % p.ka, b),
            device_id_type=MESH,
        )

    def pass_v(i):
        source = (a + p.ka - i) % p.ka
        part = pl.ds(source * p.local_k + core * half, half)
        return pltpu.make_async_remote_copy(
            src_ref=vg.at[part],
            dst_ref=vg.at[part],
            send_sem=f_sem.at[i],
            recv_sem=v2_sem.at[i],
            device_id=(a, sibling),
            device_id_type=MESH,
        )

    for i in range(1, p.ka):
        send_v(i).start()

    def right_side(k, carry):
        @pl.when(k + 1 < p.local_k)
        def _():
            load_g(k + 1).start()

        load_g(k).wait()
        g = gbuf[k % 2]
        g = jnp.concatenate([g[0], g[1]], axis=-1).reshape(p.local_q * p.bands, LANES)
        g_high, g_low = split(g)
        r_high, r_low = split(right[k])
        h = dot(
            jnp.concatenate([g_high, g_low], axis=1), jnp.concatenate([r_high, r_high], axis=0)
        ) + dot(g_high, r_low)
        h = h.reshape(p.local_q, p.bands, LANES)
        for q in range(p.local_q):
            rot[k, pl.ds(q, p.bands, stride=p.local_q), :] = h[q]
        return carry

    lax.fori_loop(0, half, right_side, 0)
    for i in range(1, p.ka):
        send_v(i).wait_recv()
        pass_v(i).start()
    lax.fori_loop(half, p.local_k, right_side, 0)
    own_v.wait()
    for i in range(1, p.ka):
        pass_v(i).wait_recv()

    def left_side(k, carry):
        for q in range(p.local_q):
            v_high, v_low = split(vg[kq[k * p.local_q + q]])
            h = rot[k, pl.ds(q, p.bands, stride=p.local_q), :]
            h_high, h_low = split(jnp.concatenate([h, swap(h, sign)], axis=0))
            rot[k, pl.ds(q, p.bands, stride=p.local_q), :] = dot(
                jnp.concatenate([v_high, v_low], axis=1),
                jnp.concatenate([h_high, h_high], axis=0),
            ) + dot(v_high, h_low)
        return carry

    def send_1(c, o):
        t = (me + o) % p.devices
        ks = pl.ds(c * p.kc, p.kc)
        return pltpu.make_async_remote_copy(
            src_ref=rot.at[ks, pl.ds(t * p.share, p.share)],
            dst_ref=x_buf.at[a, ks, b],
            send_sem=s1_sem.at[c],
            recv_sem=r1_sem.at[c],
            device_id=(t // p.pb, t % p.pb),
            device_id_type=MESH,
        )

    def own_1(c):
        ks = pl.ds(c * p.kc, p.kc)
        return pltpu.make_async_copy(
            rot.at[ks, pl.ds(me * p.share, p.share)], x_buf.at[a, ks, b], r1_sem.at[c]
        )

    def sum_q(c):
        part = x_buf.at[:, pl.ds(c * p.kc, p.kc)]
        pltpu.make_async_copy(part, part, r1_sem.at[c]).wait()

        @pl.loop(0, (p.ka // 2) * p.kc)
        def _(i):
            pair = i // p.kc
            k = c * p.kc + i % p.kc
            x = jnp.concatenate(
                [
                    x_buf[2 * pair, k].reshape(p.pb * p.share, LANES),
                    x_buf[2 * pair + 1, k].reshape(p.pb * p.share, LANES),
                ],
                axis=1,
            )
            x_high, x_low = split(x)
            y = dot(tq[...], jnp.concatenate([x_high, x_high, x_low], axis=0))
            rows = p.rp_count * p.rows
            for j in range(2):
                cols = slice(j * LANES, (j + 1) * LANES)
                where = pl.ds((2 * pair + j) * p.local_k + k, rows, stride=p.k_count)
                y_buf[where, :] = y[:rows, cols] + swap(y[rows:, cols], sign)

    @pl.loop(0, p.k_chunks)
    def _(c):
        lax.fori_loop(c * p.kc, (c + 1) * p.kc, left_side, 0)

        @pl.loop(1, p.devices)
        def _(o):
            send_1(c, o).start()

        own_1(c).start()

        @pl.when(c > 0)
        def _():
            sum_q(c - 1)

    sum_q(p.k_chunks - 1)

    def send_2(j, o):
        t = (b + o) % p.pb
        first = (t * p.rp_local + j * p.rpc) * p.rows * p.k_count
        return pltpu.make_async_remote_copy(
            src_ref=y_buf.at[pl.ds(first, p.piece)],
            dst_ref=z_buf.at[j, b],
            send_sem=s2_sem.at[j],
            recv_sem=r2_sem.at[j],
            device_id=(a, t),
            device_id_type=MESH,
        )

    @pl.loop(0, p.rp_chunks)
    def _(j):
        @pl.loop(1, p.pb)
        def _(o):
            send_2(j, o).start()

        first = (b * p.rp_local + j * p.rpc) * p.rows * p.k_count
        pltpu.make_async_copy(
            y_buf.at[pl.ds(first, p.piece)], z_buf.at[j, b], r2_sem.at[j]
        ).start()

    def send_3(j, o):
        t = (a + o) % p.ka
        slot = j % p.slots
        return pltpu.make_async_remote_copy(
            src_ref=w_buf.at[slot, t],
            dst_ref=out.at[j, a],
            send_sem=s3_sem.at[slot],
            recv_sem=r3_sem.at[j],
            device_id=(t, b),
            device_id_type=MESH,
        )

    def own_3(j):
        slot = j % p.slots
        return pltpu.make_async_copy(w_buf.at[slot, a], out.at[j, a], g_sem.at[slot])

    def free_3(j):
        slot = j % p.slots
        sent = w_buf.at[slot, pl.ds(0, p.ka - 1)]
        pltpu.make_async_copy(sent, sent, s3_sem.at[slot]).wait()
        own_3(j).wait()

    @pl.loop(0, p.rp_chunks)
    def _(j):
        pltpu.make_async_copy(z_buf.at[j], z_buf.at[j], r2_sem.at[j]).wait()
        slot = j % p.slots

        @pl.when(j >= p.slots)
        def _():
            free_3(j - p.slots)

        @pl.loop(0, p.pb * p.rpc)
        def _(i):
            source = i // p.rpc
            rp = i % p.rpc
            for r in range(0, p.rows, 2):
                z = jnp.concatenate(
                    [
                        z_buf[j, source, pl.ds((rp * p.rows + r) * p.k_count, p.k_count), :],
                        z_buf[j, source, pl.ds((rp * p.rows + r + 1) * p.k_count, p.k_count), :],
                    ],
                    axis=1,
                )
                z_high, z_low = split(z)
                w = dot(tk[...], jnp.concatenate([z_high, z_high, z_low], axis=0))
                for s in range(2):
                    cols = slice(s * LANES, (s + 1) * LANES)
                    full = w[: p.re_count, cols] + swap(w[p.re_count :, cols], sign)
                    at = rp * p.width + source * p.rows + r + s
                    where = pl.ds(at, p.re_local, stride=p.rpc * p.width)
                    for t in range(p.ka):
                        w_buf[slot, t, where, :] = full[t * p.re_local : (t + 1) * p.re_local]

        @pl.loop(1, p.ka)
        def _(o):
            send_3(j, o).start()

        own_3(j).start()

    for j in range(p.rp_chunks - p.slots, p.rp_chunks):
        free_3(j)

    @pl.loop(0, p.rp_chunks)
    def _(j):
        into = out.at[j, pl.ds(0, p.ka - 1)]
        pltpu.make_async_copy(into, into, r3_sem.at[j]).wait()
        first = z_buf.at[j, pl.ds(0, p.pb - 1)]
        pltpu.make_async_copy(first, first, s2_sem.at[j]).wait()

    @pl.loop(0, p.k_chunks)
    def _(c):
        sent = rot.at[pl.ds(c * p.kc, p.kc), pl.ds(0, (p.devices - 1) * p.share)]
        pltpu.make_async_copy(sent, sent, s1_sem.at[c]).wait()

    for i in range(1, p.ka):
        send_v(i).wait_send()
        pass_v(i).wait_send()


def unpack(p, step, x_ref, o_ref):
    for t in range(p.ka):
        x = x_ref[0, t].reshape(step, p.rpc, p.width, LANES)
        o_ref[0, :, :, t * p.width : (t + 1) * p.width, :] = x[..., : p.bands]
        o_ref[1, :, :, t * p.width : (t + 1) * p.width, :] = x[..., p.bands :]


def three_parts(table):
    high = lax.reduce_precision(table, 8, 7)
    low = lax.reduce_precision(table - high, 8, 7)
    return jnp.concatenate([high, low, high], axis=1).astype(jnp.bfloat16)


def local_fused(p, bloch, gauge, kq_index, qpoint, re_vectors, re_weight, rp_vectors, rp_weight):
    real, imag = gauge[0], gauge[1]
    v_in = jnp.concatenate([jnp.swapaxes(real, 1, 2), jnp.swapaxes(imag, 1, 2)], axis=2)
    right = jnp.concatenate(
        [jnp.concatenate([real, imag], axis=2), jnp.concatenate([-imag, real], axis=2)], axis=1
    )
    vectors = jnp.repeat(rp_vectors, p.rows, axis=0)
    points = jnp.broadcast_to(
        qpoint.reshape(p.pb, 1, p.local_q), (p.pb, p.rows, p.local_q)
    ).reshape(-1)
    cosine, sine = mesh_phase(vectors, points, p.q_count)
    row = jnp.arange(p.rp_count * p.rows, dtype=jnp.int32) % p.rows
    col = jnp.arange(p.q_count * p.rows, dtype=jnp.int32) // p.local_q % p.rows
    weight = jnp.repeat(rp_weight, p.rows).astype(jnp.float32)[:, None]
    same = row[:, None] == col[None, :]
    tq = jnp.where(
        jnp.concatenate([same, same], axis=0),
        jnp.concatenate([cosine / weight, sine / weight], axis=0),
        0.0,
    )
    cosine, sine = mesh_phase(re_vectors, jnp.arange(p.k_count, dtype=jnp.int32), p.k_count)
    weight = re_weight.astype(jnp.float32)[:, None]
    tk = jnp.concatenate([cosine / weight, sine / weight], axis=0)
    tq, tk = three_parts(tq), three_parts(tk)

    f32 = jnp.float32
    dma = pltpu.SemaphoreType.DMA
    vmem = pl.BlockSpec(memory_space=pltpu.VMEM)
    any_space = pl.BlockSpec(memory_space=pl.ANY)
    landed = pl.pallas_call(
        functools.partial(kernel, p),
        out_shape=jax.ShapeDtypeStruct((p.rp_chunks, p.ka, p.block, LANES), f32),
        in_specs=[
            any_space,
            any_space,
            vmem,
            pl.BlockSpec(memory_space=pltpu.SMEM),
            vmem,
            vmem,
        ],
        out_specs=any_space,
        scratch_shapes=[
            pltpu.VMEM((2, 2, p.local_q, p.bands, p.bands), f32),
            pltpu.VMEM((p.k_count, p.bands, LANES), f32),
            pltpu.VMEM((p.local_k, p.devices * p.share, LANES), f32),
            pltpu.VMEM((p.ka, p.local_k, p.pb, p.share, LANES), f32),
            pltpu.VMEM((p.rp_count * p.rows * p.k_count, LANES), f32),
            pltpu.VMEM((p.rp_chunks, p.pb, p.piece, LANES), f32),
            pltpu.VMEM((p.slots, p.ka, p.block, LANES), f32),
            dma((2,)),
            dma,
            dma((p.ka,)),
            dma((p.ka,)),
            dma((p.ka,)),
            dma((p.ka,)),
            dma((p.k_chunks,)),
            dma((p.k_chunks,)),
            dma((p.rp_chunks,)),
            dma((p.rp_chunks,)),
            dma((p.slots,)),
            dma((p.rp_chunks,)),
        ],
        compiler_params=pltpu.CompilerParams(
            collective_id=0, has_side_effects=True, vmem_limit_bytes=VMEM_BYTES
        ),
    )(bloch, v_in, right, kq_index.reshape(-1), tq, tk)

    step = 8
    return pl.pallas_call(
        functools.partial(unpack, p, step),
        grid=(p.re_local // step, p.rp_chunks),
        out_shape=jax.ShapeDtypeStruct((2, p.re_local, p.rp_local, p.bands, p.bands), f32),
        in_specs=[
            pl.BlockSpec(
                (1, p.ka, step * p.rpc * p.width, LANES), lambda i, j: (j, 0, i, 0)
            )
        ],
        out_specs=pl.BlockSpec(
            (2, step, p.rpc, p.bands, p.bands), lambda i, j: (0, i, j, 0, 0)
        ),
    )(landed)


def local(bloch_elements, gauge, kq_index, qpoint, re_vectors, re_weight, rp_vectors, rp_weight):
    p = Plan(
        lax.axis_size("ka"),
        lax.axis_size("pb"),
        bloch_elements.shape[1],
        bloch_elements.shape[2],
        bloch_elements.shape[3],
        re_vectors.shape[0],
        rp_vectors.shape[0],
    )
    program = functools.partial(local_fused, p) if p.fits else local_general
    return program(
        bloch_elements, gauge, kq_index, qpoint, re_vectors, re_weight, rp_vectors, rp_weight
    )


def solution(mesh):
    placed = (
        P(None, "ka", "pb", None, None),
        P(None, "ka", None, None),
        P("ka", "pb"),
        P(),
        P(),
        P(),
        P(),
        P(),
    )
    return jax.shard_map(
        local,
        mesh=mesh,
        in_specs=placed,
        out_specs=P(None, "ka", "pb", None, None),
        check_vma=False,
    )
```

```python
import functools
import math

import jax
import jax.numpy as jnp
from jax import lax
from jax.experimental import pallas as pl
from jax.experimental.pallas import tpu as pltpu
from jax.sharding import PartitionSpec as P

MK1 = 4
MK2 = 6
MK3 = 4
LANES = 128
VMEM_BYTES = 67_000_000
MESH = pl.DeviceIdType.MESH


def mesh_phase(vectors, points, total_count):
    first_index = points // (MK2 * MK3)
    second_index = points // MK3 % MK2
    third_index = points % MK3
    phase_turns = (
        vectors[:, 0:1] * (first_index * (MK2 * MK3))[None, :]
        + vectors[:, 1:2] * (second_index * (MK1 * MK3))[None, :]
        + vectors[:, 2:3] * (third_index * (MK1 * MK2))[None, :]
    )
    phase_turns = jnp.mod(phase_turns, MK1 * MK2 * MK3)
    angles = phase_turns.astype(jnp.float32) * (2.0 * math.pi / (MK1 * MK2 * MK3))
    return (jnp.cos(angles) / total_count, jnp.sin(angles) / total_count)


def rotate_gauge(elements, left_side, right_side):
    exact_mode = lax.Precision.HIGH
    real_part = jnp.matmul(elements[0], right_side[0], precision=exact_mode) - jnp.matmul(
        elements[1], right_side[1], precision=exact_mode
    )
    imag_part = jnp.matmul(elements[0], right_side[1], precision=exact_mode) + jnp.matmul(
        elements[1], right_side[0], precision=exact_mode
    )
    left_real = jnp.swapaxes(left_side[0], -1, -2)
    left_imag = jnp.swapaxes(left_side[1], -1, -2)
    rot_real = jnp.matmul(left_real, real_part, precision=exact_mode) + jnp.matmul(
        left_imag, imag_part, precision=exact_mode
    )
    rot_imag = jnp.matmul(left_real, imag_part, precision=exact_mode) - jnp.matmul(
        left_imag, real_part, precision=exact_mode
    )
    return jnp.stack([rot_real, rot_imag])


def complex_table(table, count):
    cosine, sine_table = table
    real_rows = jnp.stack([cosine, sine_table], axis=1)
    imag_rows = jnp.stack([-sine_table, cosine], axis=1)
    scale = count.astype(jnp.float32)[None, :, None, None]
    return jnp.stack([real_rows, imag_rows]) / scale


def local_general(bloch_elements, gauge, kq_index, qpoint, re_vectors, re_weight, rp_vectors, rp_weight):
    local_k = bloch_elements.shape[1]
    local_q = bloch_elements.shape[2]
    bands = bloch_elements.shape[3]
    pairs = bands * bands
    gathered = lax.all_gather(gauge, "ka", axis=1, tiled=True)
    left_side = jnp.take(gathered, kq_index, axis=1)
    rotated = rotate_gauge(bloch_elements, left_side, gauge[:, :, None])
    rotated = rotated.reshape(2, local_k, local_q, pairs)
    k_count = gathered.shape[1]
    q_count = qpoint.shape[0]
    k_table = mesh_phase(re_vectors, jnp.arange(k_count, dtype=jnp.int32), k_count)
    q_table = mesh_phase(rp_vectors, qpoint, q_count)
    ka_count = lax.axis_size("ka")
    pb_count = lax.axis_size("pb")
    re_local = re_vectors.shape[0] // ka_count
    rp_local = rp_vectors.shape[0] // pb_count
    devices = ka_count * pb_count
    column_width = pairs // devices
    leaving = rotated.reshape(2, local_k, local_q, devices, column_width).transpose(3, 0, 1, 2, 4)
    leaving = leaving.reshape(devices, 2 * local_k * local_q, column_width)
    joined = lax.all_to_all(leaving, ("ka", "pb"), split_axis=0, concat_axis=0, tiled=True)
    joined = joined.reshape(ka_count, pb_count, 2, local_k, local_q, column_width)
    k_blocks = complex_table(k_table, re_weight).reshape(
        2, ka_count, re_local, 2, ka_count, local_k
    )
    q_blocks = complex_table(q_table, rp_weight).reshape(
        2, pb_count, rp_local, 2, pb_count, local_q
    )
    exact_mode = lax.Precision.HIGH
    electron = jnp.einsum("dauemk,mpeklx->dauplx", k_blocks, joined, precision=exact_mode)
    spread = jnp.einsum("fbvdpl,dauplx->abfuvx", q_blocks, electron, precision=exact_mode)
    spread = spread.reshape(devices, 2 * re_local * rp_local, column_width)
    result = lax.all_to_all(spread, ("ka", "pb"), split_axis=0, concat_axis=0, tiled=True)
    result = result.reshape(devices, 2, re_local, rp_local, column_width)
    return result.transpose(1, 2, 3, 0, 4).reshape(2, re_local, rp_local, bands, bands)


def split(x):
    high = x.astype(jnp.bfloat16)
    low = (x - high.astype(jnp.float32)).astype(jnp.bfloat16)
    return high, low


def dot(a, b):
    return jnp.dot(a, b, preferred_element_type=jnp.float32)


def swap(x, sign):
    return pltpu.roll(x, x.shape[-1] // 2, x.ndim - 1) * sign


class Plan:
    def __init__(self, ka, pb, local_k, local_q, bands, re_count, rp_count):
        self.ka, self.pb = ka, pb
        self.devices = ka * pb
        self.local_k, self.local_q, self.bands = local_k, local_q, bands
        self.k_count, self.q_count = ka * local_k, pb * local_q
        self.re_count, self.rp_count = re_count, rp_count
        self.re_local, self.rp_local = re_count // ka, rp_count // pb
        self.fits = (
            2 * bands == LANES
            and bands % self.devices == 0
            and pb & (pb - 1) == 0
            and pb > 1
            and ka % 2 == 0
            and local_k % 6 == 0
        )
        if not self.fits:
            return
        self.rows = bands // self.devices
        self.share = self.rows * local_q
        self.kc = 3
        self.k_chunks = local_k // self.kc
        self.rpc = 1
        self.rp_chunks = self.rp_local // self.rpc
        self.width = self.rows * pb
        self.piece = self.rpc * self.rows * self.k_count
        self.block = self.re_local * self.rpc * self.width
        self.slots = 4
        self.ahead = 2
        self.fits = (
            self.share % 8 == 0
            and self.k_count % 16 == 0
            and (pb * self.share) % 16 == 0
            and self.width % 8 == 0
            and self.rp_local % self.rpc == 0
            and self.rp_chunks > self.slots
        )


def kernel(
    p,
    bloch,
    v_in,
    right,
    kq,
    tq,
    tk,
    out,
    gbuf,
    vg,
    rot,
    x_buf,
    y_buf,
    z_buf,
    w_buf,
    g_sem,
    own_sem,
    vs_sem,
    v1_sem,
    f_sem,
    v2_sem,
    s1_sem,
    r1_sem,
    s2_sem,
    r2_sem,
    s3_sem,
    r3_sem,
):
    a = lax.axis_index("ka")
    b = lax.axis_index("pb")
    me = a * p.pb + b
    core = b % 2
    sibling = b + 1 - 2 * core
    half = p.local_k // 2
    lane = lax.broadcasted_iota(jnp.int32, (1, LANES), 1)
    sign = jnp.where(lane < p.bands, 1.0, -1.0).astype(jnp.float32)

    def partner(o):
        t, bit = 0, 1
        while bit < p.pb:
            t = t + (b // bit + o // bit) % 2 * bit
            bit *= 2
        return t

    def load_g(k):
        return pltpu.make_async_copy(bloch.at[:, k], gbuf.at[k % 2], g_sem.at[k % 2])

    load_g(0).start()
    own_v = pltpu.make_async_copy(v_in, vg.at[pl.ds(a * p.local_k, p.local_k)], own_sem)
    own_v.start()

    barrier = pltpu.get_barrier_semaphore()

    @pl.loop(1, p.devices)
    def _(o):
        t = (me + o) % p.devices
        pl.semaphore_signal(barrier, inc=1, device_id=(t // p.pb, t % p.pb), device_id_type=MESH)

    pl.semaphore_wait(barrier, p.devices - 1)

    def send_v(i):
        return pltpu.make_async_remote_copy(
            src_ref=v_in.at[pl.ds(core * half, half)],
            dst_ref=vg.at[pl.ds(a * p.local_k + core * half, half)],
            send_sem=vs_sem.at[i],
            recv_sem=v1_sem.at[i],
            device_id=((a + i) % p.ka, b),
            device_id_type=MESH,
        )

    def pass_v(i):
        source = (a + p.ka - i) % p.ka
        part = pl.ds(source * p.local_k + core * half, half)
        return pltpu.make_async_remote_copy(
            src_ref=vg.at[part],
            dst_ref=vg.at[part],
            send_sem=f_sem.at[i],
            recv_sem=v2_sem.at[i],
            device_id=(a, sibling),
            device_id_type=MESH,
        )

    for i in range(1, p.ka):
        send_v(i).start()

    def right_side(k, carry):
        @pl.when(k + 1 < p.local_k)
        def _():
            load_g(k + 1).start()

        load_g(k).wait()
        g = gbuf[k % 2]
        g = jnp.concatenate([g[0], g[1]], axis=-1).reshape(p.local_q * p.bands, LANES)
        g_high, g_low = split(g)
        r_high, r_low = split(right[k])
        h = dot(
            jnp.concatenate([g_high, g_low], axis=1), jnp.concatenate([r_high, r_high], axis=0)
        ) + dot(g_high, r_low)
        h = h.reshape(p.local_q, p.bands, LANES)
        for q in range(p.local_q):
            rot[k, pl.ds(q, p.bands, stride=p.local_q), :] = h[q]
        return carry

    lax.fori_loop(0, half, right_side, 0)
    for i in range(1, p.ka):
        send_v(i).wait_recv()
        pass_v(i).start()
    lax.fori_loop(half, p.local_k, right_side, 0)
    own_v.wait()
    for i in range(1, p.ka):
        pass_v(i).wait_recv()

    def left_side(k, carry):
        for q in range(p.local_q):
            v_high, v_low = split(vg[kq[k * p.local_q + q]])
            h = rot[k, pl.ds(q, p.bands, stride=p.local_q), :]
            h_high, h_low = split(jnp.concatenate([h, swap(h, sign)], axis=0))
            rot[k, pl.ds(q, p.bands, stride=p.local_q), :] = dot(
                jnp.concatenate([v_high, v_low], axis=1),
                jnp.concatenate([h_high, h_high], axis=0),
            ) + dot(v_high, h_low)
        return carry

    def send_1(c, n):
        ta = (a + p.ka - 1 - n % p.ka) % p.ka
        tb = partner(p.pb - 1 - n // p.ka)
        t = ta * p.pb + tb
        ks = pl.ds(c * p.kc, p.kc)
        return pltpu.make_async_remote_copy(
            src_ref=rot.at[ks, pl.ds(t * p.share, p.share)],
            dst_ref=x_buf.at[a, ks, b],
            send_sem=s1_sem.at[c],
            recv_sem=r1_sem.at[c],
            device_id=(ta, tb),
            device_id_type=MESH,
        )

    def own_1(c):
        ks = pl.ds(c * p.kc, p.kc)
        return pltpu.make_async_copy(
            rot.at[ks, pl.ds(me * p.share, p.share)], x_buf.at[a, ks, b], r1_sem.at[c]
        )

    def sum_q(c):
        part = x_buf.at[:, pl.ds(c * p.kc, p.kc)]
        pltpu.make_async_copy(part, part, r1_sem.at[c]).wait()

        @pl.loop(0, (p.ka // 2) * p.kc)
        def _(i):
            pair = i // p.kc
            k = c * p.kc + i % p.kc
            x = jnp.concatenate(
                [
                    x_buf[2 * pair, k].reshape(p.pb * p.share, LANES),
                    x_buf[2 * pair + 1, k].reshape(p.pb * p.share, LANES),
                ],
                axis=1,
            )
            x_high, x_low = split(x)
            y = dot(tq[...], jnp.concatenate([x_high, x_high, x_low], axis=0))
            rows = p.rp_count * p.rows
            for j in range(2):
                cols = slice(j * LANES, (j + 1) * LANES)
                where = pl.ds((2 * pair + j) * p.local_k + k, rows, stride=p.k_count)
                y_buf[where, :] = y[:rows, cols] + swap(y[rows:, cols], sign)

    @pl.loop(0, p.k_chunks)
    def _(c):
        lax.fori_loop(c * p.kc, (c + 1) * p.kc, left_side, 0)

        @pl.loop(0, p.devices - 1)
        def _(n):
            send_1(c, n).start()

        own_1(c).start()

        @pl.when(c > 0)
        def _():
            sum_q(c - 1)

    sum_q(p.k_chunks - 1)

    def send_2(j, o):
        t = partner(o)
        first = (t * p.rp_local + j * p.rpc) * p.rows * p.k_count
        return pltpu.make_async_remote_copy(
            src_ref=y_buf.at[pl.ds(first, p.piece)],
            dst_ref=z_buf.at[j, b],
            send_sem=s2_sem.at[j],
            recv_sem=r2_sem.at[j],
            device_id=(a, t),
            device_id_type=MESH,
        )

    def start_2(j):
        @pl.loop(1, p.pb)
        def _(o):
            send_2(j, o).start()

        first = (b * p.rp_local + j * p.rpc) * p.rows * p.k_count
        pltpu.make_async_copy(
            y_buf.at[pl.ds(first, p.piece)], z_buf.at[j, b], r2_sem.at[j]
        ).start()

    for j in range(p.ahead):
        start_2(j)

    def send_3(j, o):
        t = (a + o) % p.ka
        slot = j % p.slots
        return pltpu.make_async_remote_copy(
            src_ref=w_buf.at[slot, t],
            dst_ref=out.at[j, a],
            send_sem=s3_sem.at[slot],
            recv_sem=r3_sem.at[j],
            device_id=(t, b),
            device_id_type=MESH,
        )

    def own_3(j):
        slot = j % p.slots
        return pltpu.make_async_copy(w_buf.at[slot, a], out.at[j, a], g_sem.at[slot])

    def free_3(j):
        slot = j % p.slots
        sent = w_buf.at[slot, pl.ds(0, p.ka - 1)]
        pltpu.make_async_copy(sent, sent, s3_sem.at[slot]).wait()
        own_3(j).wait()

    @pl.loop(0, p.rp_chunks)
    def _(j):
        pltpu.make_async_copy(z_buf.at[j], z_buf.at[j], r2_sem.at[j]).wait()
        slot = j % p.slots

        @pl.when(j + p.ahead < p.rp_chunks)
        def _():
            start_2(j + p.ahead)

        @pl.when(j >= p.slots)
        def _():
            free_3(j - p.slots)

        @pl.loop(0, p.pb * p.rpc)
        def _(i):
            source = i // p.rpc
            rp = i % p.rpc
            for r in range(0, p.rows, 2):
                z = jnp.concatenate(
                    [
                        z_buf[j, source, pl.ds((rp * p.rows + r) * p.k_count, p.k_count), :],
                        z_buf[j, source, pl.ds((rp * p.rows + r + 1) * p.k_count, p.k_count), :],
                    ],
                    axis=1,
                )
                z_high, z_low = split(z)
                w = dot(tk[...], jnp.concatenate([z_high, z_high, z_low], axis=0))
                for s in range(2):
                    cols = slice(s * LANES, (s + 1) * LANES)
                    full = w[: p.re_count, cols] + swap(w[p.re_count :, cols], sign)
                    at = rp * p.width + source * p.rows + r + s
                    where = pl.ds(at, p.re_local, stride=p.rpc * p.width)
                    for t in range(p.ka):
                        w_buf[slot, t, where, :] = full[t * p.re_local : (t + 1) * p.re_local]

        @pl.loop(1, p.ka)
        def _(o):
            send_3(j, o).start()

        own_3(j).start()

    for j in range(p.rp_chunks - p.slots, p.rp_chunks):
        free_3(j)

    @pl.loop(0, p.rp_chunks)
    def _(j):
        into = out.at[j, pl.ds(0, p.ka - 1)]
        pltpu.make_async_copy(into, into, r3_sem.at[j]).wait()
        first = z_buf.at[j, pl.ds(0, p.pb - 1)]
        pltpu.make_async_copy(first, first, s2_sem.at[j]).wait()

    @pl.loop(0, p.k_chunks)
    def _(c):
        sent = rot.at[pl.ds(c * p.kc, p.kc), pl.ds(0, (p.devices - 1) * p.share)]
        pltpu.make_async_copy(sent, sent, s1_sem.at[c]).wait()

    for i in range(1, p.ka):
        send_v(i).wait_send()
        pass_v(i).wait_send()


def unpack(p, step, x_ref, o_ref):
    for t in range(p.ka):
        x = x_ref[0, t].reshape(step, p.rpc, p.width, LANES)
        o_ref[0, :, :, t * p.width : (t + 1) * p.width, :] = x[..., : p.bands]
        o_ref[1, :, :, t * p.width : (t + 1) * p.width, :] = x[..., p.bands :]


def three_parts(table):
    high = lax.reduce_precision(table, 8, 7)
    low = lax.reduce_precision(table - high, 8, 7)
    return jnp.concatenate([high, low, high], axis=1).astype(jnp.bfloat16)


def local_fused(p, bloch, gauge, kq_index, qpoint, re_vectors, re_weight, rp_vectors, rp_weight):
    real, imag = gauge[0], gauge[1]
    v_in = jnp.concatenate([jnp.swapaxes(real, 1, 2), jnp.swapaxes(imag, 1, 2)], axis=2)
    right = jnp.concatenate(
        [jnp.concatenate([real, imag], axis=2), jnp.concatenate([-imag, real], axis=2)], axis=1
    )
    vectors = jnp.repeat(rp_vectors, p.rows, axis=0)
    points = jnp.broadcast_to(
        qpoint.reshape(p.pb, 1, p.local_q), (p.pb, p.rows, p.local_q)
    ).reshape(-1)
    cosine, sine = mesh_phase(vectors, points, p.q_count)
    row = jnp.arange(p.rp_count * p.rows, dtype=jnp.int32) % p.rows
    col = jnp.arange(p.q_count * p.rows, dtype=jnp.int32) // p.local_q % p.rows
    weight = jnp.repeat(rp_weight, p.rows).astype(jnp.float32)[:, None]
    same = row[:, None] == col[None, :]
    tq = jnp.where(
        jnp.concatenate([same, same], axis=0),
        jnp.concatenate([cosine / weight, sine / weight], axis=0),
        0.0,
    )
    cosine, sine = mesh_phase(re_vectors, jnp.arange(p.k_count, dtype=jnp.int32), p.k_count)
    weight = re_weight.astype(jnp.float32)[:, None]
    tk = jnp.concatenate([cosine / weight, sine / weight], axis=0)
    tq, tk = three_parts(tq), three_parts(tk)

    f32 = jnp.float32
    dma = pltpu.SemaphoreType.DMA
    vmem = pl.BlockSpec(memory_space=pltpu.VMEM)
    any_space = pl.BlockSpec(memory_space=pl.ANY)
    landed = pl.pallas_call(
        functools.partial(kernel, p),
        out_shape=jax.ShapeDtypeStruct((p.rp_chunks, p.ka, p.block, LANES), f32),
        in_specs=[
            any_space,
            any_space,
            vmem,
            pl.BlockSpec(memory_space=pltpu.SMEM),
            vmem,
            vmem,
        ],
        out_specs=any_space,
        scratch_shapes=[
            pltpu.VMEM((2, 2, p.local_q, p.bands, p.bands), f32),
            pltpu.VMEM((p.k_count, p.bands, LANES), f32),
            pltpu.VMEM((p.local_k, p.devices * p.share, LANES), f32),
            pltpu.VMEM((p.ka, p.local_k, p.pb, p.share, LANES), f32),
            pltpu.VMEM((p.rp_count * p.rows * p.k_count, LANES), f32),
            pltpu.VMEM((p.rp_chunks, p.pb, p.piece, LANES), f32),
            pltpu.VMEM((p.slots, p.ka, p.block, LANES), f32),
            dma((max(2, p.slots),)),
            dma,
            dma((p.ka,)),
            dma((p.ka,)),
            dma((p.ka,)),
            dma((p.ka,)),
            dma((p.k_chunks,)),
            dma((p.k_chunks,)),
            dma((p.rp_chunks,)),
            dma((p.rp_chunks,)),
            dma((p.slots,)),
            dma((p.rp_chunks,)),
        ],
        compiler_params=pltpu.CompilerParams(
            collective_id=0, has_side_effects=True, vmem_limit_bytes=VMEM_BYTES
        ),
    )(bloch, v_in, right, kq_index.reshape(-1), tq, tk)

    step = p.re_local
    return pl.pallas_call(
        functools.partial(unpack, p, step),
        grid=(p.re_local // step, p.rp_chunks),
        out_shape=jax.ShapeDtypeStruct((2, p.re_local, p.rp_local, p.bands, p.bands), f32),
        in_specs=[
            pl.BlockSpec(
                (1, p.ka, step * p.rpc * p.width, LANES), lambda i, j: (j, 0, i, 0)
            )
        ],
        out_specs=pl.BlockSpec(
            (2, step, p.rpc, p.bands, p.bands), lambda i, j: (0, i, j, 0, 0)
        ),
    )(landed)


def local(bloch_elements, gauge, kq_index, qpoint, re_vectors, re_weight, rp_vectors, rp_weight):
    p = Plan(
        lax.axis_size("ka"),
        lax.axis_size("pb"),
        bloch_elements.shape[1],
        bloch_elements.shape[2],
        bloch_elements.shape[3],
        re_vectors.shape[0],
        rp_vectors.shape[0],
    )
    program = functools.partial(local_fused, p) if p.fits else local_general
    return program(
        bloch_elements, gauge, kq_index, qpoint, re_vectors, re_weight, rp_vectors, rp_weight
    )


def solution(mesh):
    placed = (
        P(None, "ka", "pb", None, None),
        P(None, "ka", None, None),
        P("ka", "pb"),
        P(),
        P(),
        P(),
        P(),
        P(),
    )
    return jax.shard_map(
        local,
        mesh=mesh,
        in_specs=placed,
        out_specs=P(None, "ka", "pb", None, None),
        check_vma=False,
    )
```

```python
import functools
import math

import jax
import jax.numpy as jnp
from jax import lax
from jax.experimental import pallas as pl
from jax.experimental.pallas import tpu as pltpu
from jax.sharding import PartitionSpec as P

MK1 = 4
MK2 = 6
MK3 = 4
LANES = 128
VMEM_BYTES = 67_000_000
MESH = pl.DeviceIdType.MESH


def mesh_phase(vectors, points, total_count):
    first_index = points // (MK2 * MK3)
    second_index = points // MK3 % MK2
    third_index = points % MK3
    phase_turns = (
        vectors[:, 0:1] * (first_index * (MK2 * MK3))[None, :]
        + vectors[:, 1:2] * (second_index * (MK1 * MK3))[None, :]
        + vectors[:, 2:3] * (third_index * (MK1 * MK2))[None, :]
    )
    phase_turns = jnp.mod(phase_turns, MK1 * MK2 * MK3)
    angles = phase_turns.astype(jnp.float32) * (2.0 * math.pi / (MK1 * MK2 * MK3))
    return (jnp.cos(angles) / total_count, jnp.sin(angles) / total_count)


def rotate_gauge(elements, left_side, right_side):
    exact_mode = lax.Precision.HIGH
    real_part = jnp.matmul(elements[0], right_side[0], precision=exact_mode) - jnp.matmul(
        elements[1], right_side[1], precision=exact_mode
    )
    imag_part = jnp.matmul(elements[0], right_side[1], precision=exact_mode) + jnp.matmul(
        elements[1], right_side[0], precision=exact_mode
    )
    left_real = jnp.swapaxes(left_side[0], -1, -2)
    left_imag = jnp.swapaxes(left_side[1], -1, -2)
    rot_real = jnp.matmul(left_real, real_part, precision=exact_mode) + jnp.matmul(
        left_imag, imag_part, precision=exact_mode
    )
    rot_imag = jnp.matmul(left_real, imag_part, precision=exact_mode) - jnp.matmul(
        left_imag, real_part, precision=exact_mode
    )
    return jnp.stack([rot_real, rot_imag])


def complex_table(table, count):
    cosine, sine_table = table
    real_rows = jnp.stack([cosine, sine_table], axis=1)
    imag_rows = jnp.stack([-sine_table, cosine], axis=1)
    scale = count.astype(jnp.float32)[None, :, None, None]
    return jnp.stack([real_rows, imag_rows]) / scale


def local_general(bloch_elements, gauge, kq_index, qpoint, re_vectors, re_weight, rp_vectors, rp_weight):
    local_k = bloch_elements.shape[1]
    local_q = bloch_elements.shape[2]
    bands = bloch_elements.shape[3]
    pairs = bands * bands
    gathered = lax.all_gather(gauge, "ka", axis=1, tiled=True)
    left_side = jnp.take(gathered, kq_index, axis=1)
    rotated = rotate_gauge(bloch_elements, left_side, gauge[:, :, None])
    rotated = rotated.reshape(2, local_k, local_q, pairs)
    k_count = gathered.shape[1]
    q_count = qpoint.shape[0]
    k_table = mesh_phase(re_vectors, jnp.arange(k_count, dtype=jnp.int32), k_count)
    q_table = mesh_phase(rp_vectors, qpoint, q_count)
    ka_count = lax.axis_size("ka")
    pb_count = lax.axis_size("pb")
    re_local = re_vectors.shape[0] // ka_count
    rp_local = rp_vectors.shape[0] // pb_count
    devices = ka_count * pb_count
    column_width = pairs // devices
    leaving = rotated.reshape(2, local_k, local_q, devices, column_width).transpose(3, 0, 1, 2, 4)
    leaving = leaving.reshape(devices, 2 * local_k * local_q, column_width)
    joined = lax.all_to_all(leaving, ("ka", "pb"), split_axis=0, concat_axis=0, tiled=True)
    joined = joined.reshape(ka_count, pb_count, 2, local_k, local_q, column_width)
    k_blocks = complex_table(k_table, re_weight).reshape(
        2, ka_count, re_local, 2, ka_count, local_k
    )
    q_blocks = complex_table(q_table, rp_weight).reshape(
        2, pb_count, rp_local, 2, pb_count, local_q
    )
    exact_mode = lax.Precision.HIGH
    electron = jnp.einsum("dauemk,mpeklx->dauplx", k_blocks, joined, precision=exact_mode)
    spread = jnp.einsum("fbvdpl,dauplx->abfuvx", q_blocks, electron, precision=exact_mode)
    spread = spread.reshape(devices, 2 * re_local * rp_local, column_width)
    result = lax.all_to_all(spread, ("ka", "pb"), split_axis=0, concat_axis=0, tiled=True)
    result = result.reshape(devices, 2, re_local, rp_local, column_width)
    return result.transpose(1, 2, 3, 0, 4).reshape(2, re_local, rp_local, bands, bands)


def split(x):
    high = x.astype(jnp.bfloat16)
    low = (x - high.astype(jnp.float32)).astype(jnp.bfloat16)
    return high, low


def dot(a, b):
    return jnp.dot(a, b, preferred_element_type=jnp.float32)


def swap(x, sign):
    return pltpu.roll(x, x.shape[-1] // 2, x.ndim - 1) * sign


class Plan:
    def __init__(self, ka, pb, local_k, local_q, bands, re_count, rp_count):
        self.ka, self.pb, self.half = ka, pb, pb // 2
        self.devices = ka * pb
        self.local_k, self.local_q, self.bands = local_k, local_q, bands
        self.k_count, self.q_count = ka * local_k, pb * local_q
        self.re_count, self.rp_count = re_count, rp_count
        self.re_local, self.rp_local = re_count // ka, rp_count // pb
        self.fits = (
            2 * bands == LANES
            and bands % self.devices == 0
            and pb & (pb - 1) == 0
            and pb > 2
            and ka % 2 == 0
            and local_k % 6 == 0
        )
        if not self.fits:
            return
        self.kb = local_k // 3
        self.kn = local_k - self.kb
        self.kc = 2
        self.steps = self.kb
        self.rows = bands // self.devices
        self.share = self.rows * local_q
        self.wide = 2 * self.share
        self.width = self.rows * pb
        self.piece = self.rows * ka * self.kn
        self.sources = pb + self.half
        self.block = self.re_local * self.width
        self.raw_ahead = min(3, self.kb)
        self.g_slots = 3
        self.slots = 2
        self.ahead = 2
        self.fits = (
            self.share % 8 == 0
            and self.k_count % 16 == 0
            and self.kb % 2 == 0
            and (ka * self.kb) % 8 == 0
            and (pb * self.share) % 16 == 0
            and self.width % 8 == 0
            and self.rp_local > self.slots
        )


def kernel(
    p,
    bloch,
    v_in,
    right,
    kq,
    kq_far,
    tq,
    tf,
    tk,
    out,
    gbuf,
    vg,
    rot,
    far,
    x_buf,
    xf_buf,
    y_buf,
    z_buf,
    w_buf,
    g_sem,
    own_sem,
    vs_sem,
    v1_sem,
    f_sem,
    v2_sem,
    s0_sem,
    r0_sem,
    s1_sem,
    r1_sem,
    sf_sem,
    rf_sem,
    s2_sem,
    r2_sem,
    s3_sem,
    r3_sem,
):
    a = lax.axis_index("ka")
    b = lax.axis_index("pb")
    core = b % 2
    sibling = b + 1 - 2 * core
    side = b // p.half
    seat = b % p.half
    other = seat + (1 - side) * p.half
    middle = p.local_k // 2
    lane = lax.broadcasted_iota(jnp.int32, (1, LANES), 1)
    sign = jnp.where(lane < p.bands, 1.0, -1.0).astype(jnp.float32)

    def xor(x, o, count):
        t, bit = 0, 1
        while bit < count:
            t = t + (x // bit + o // bit) % 2 * bit
            bit *= 2
        return t

    def load_g(k):
        slot = k % p.g_slots
        return pltpu.make_async_copy(bloch.at[:, k], gbuf.at[slot], g_sem.at[slot])

    for k in range(p.g_slots):
        load_g(k).start()
    own_v = pltpu.make_async_copy(v_in, vg.at[pl.ds(a * p.local_k, p.local_k)], own_sem)
    own_v.start()

    barrier = pltpu.get_barrier_semaphore()
    me = a * p.pb + b

    @pl.loop(1, p.devices)
    def _(o):
        t = (me + o) % p.devices
        pl.semaphore_signal(barrier, inc=1, device_id=(t // p.pb, t % p.pb), device_id_type=MESH)

    pl.semaphore_wait(barrier, p.devices - 1)

    def send_v(i):
        return pltpu.make_async_remote_copy(
            src_ref=v_in.at[pl.ds(core * middle, middle)],
            dst_ref=vg.at[pl.ds(a * p.local_k + core * middle, middle)],
            send_sem=vs_sem.at[i],
            recv_sem=v1_sem.at[i],
            device_id=((a + i) % p.ka, b),
            device_id_type=MESH,
        )

    def pass_v(i):
        source = (a + p.ka - i) % p.ka
        part = pl.ds(source * p.local_k + core * middle, middle)
        return pltpu.make_async_remote_copy(
            src_ref=vg.at[part],
            dst_ref=vg.at[part],
            send_sem=f_sem.at[i],
            recv_sem=v2_sem.at[i],
            device_id=(a, sibling),
            device_id_type=MESH,
        )

    for i in range(1, p.ka):
        send_v(i).start()

    def right_side(k, carry):
        load_g(k).wait()
        g = gbuf[k % p.g_slots]
        g = jnp.concatenate([g[0], g[1]], axis=-1).reshape(p.local_q * p.bands, LANES)
        g_high, g_low = split(g)
        r_high, r_low = split(right[k])
        h = dot(
            jnp.concatenate([g_high, g_low], axis=1), jnp.concatenate([r_high, r_high], axis=0)
        ) + dot(g_high, r_low)
        h = h.reshape(p.local_q, p.bands, LANES)
        for q in range(p.local_q):
            rot[k, pl.ds(q, p.bands, stride=p.local_q), :] = h[q]

        @pl.when(k + p.g_slots < p.local_k)
        def _():
            load_g(k + p.g_slots).start()

        return carry

    def send_0(k):
        return pltpu.make_async_remote_copy(
            src_ref=rot.at[k],
            dst_ref=far.at[k],
            send_sem=s0_sem.at[k],
            recv_sem=r0_sem.at[k],
            device_id=(a, other),
            device_id_type=MESH,
        )

    @pl.loop(0, p.raw_ahead)
    def _(k):
        right_side(k, 0)
        send_0(k).start()

    lax.fori_loop(p.raw_ahead, middle, right_side, 0)
    for i in range(1, p.ka):
        send_v(i).wait_recv()
        pass_v(i).start()
    lax.fori_loop(middle, p.local_k, right_side, 0)
    own_v.wait()
    for i in range(1, p.ka):
        pass_v(i).wait_recv()

    def left_side(buf, k, index, first):
        for q in range(p.local_q):
            v_high, v_low = split(vg[index[first + q]])
            h = buf[k, pl.ds(q, p.bands, stride=p.local_q), :]
            h_high, h_low = split(jnp.concatenate([h, swap(h, sign)], axis=0))
            buf[k, pl.ds(q, p.bands, stride=p.local_q), :] = dot(
                jnp.concatenate([v_high, v_low], axis=1),
                jnp.concatenate([h_high, h_high], axis=0),
            ) + dot(v_high, h_low)

    def send_1(c, n):
        ta = (a + p.ka - 1 - n % p.ka) % p.ka
        tb = xor(b, p.pb - 1 - n // p.ka, p.pb)
        t = ta * p.pb + tb
        return pltpu.make_async_remote_copy(
            src_ref=rot.at[pl.ds(p.kb + c * p.kc, p.kc), pl.ds(t * p.share, p.share)],
            dst_ref=x_buf.at[a, pl.ds(c * p.kc, p.kc), b],
            send_sem=s1_sem.at[c],
            recv_sem=r1_sem.at[c],
            device_id=(ta, tb),
            device_id_type=MESH,
        )

    def own_1(c):
        return pltpu.make_async_copy(
            rot.at[pl.ds(p.kb + c * p.kc, p.kc), pl.ds(me * p.share, p.share)],
            x_buf.at[a, pl.ds(c * p.kc, p.kc), b],
            r1_sem.at[c],
        )

    def send_f(buf, k, came_from, n):
        ta = (a + p.ka - 1 - n % p.ka) % p.ka
        ts = xor(seat, p.half - 1 - n // p.ka, p.half)
        t = ta * p.half + ts
        return pltpu.make_async_remote_copy(
            src_ref=buf.at[k, pl.ds(t * p.wide, p.wide)],
            dst_ref=xf_buf.at[a, k, came_from],
            send_sem=sf_sem.at[k],
            recv_sem=rf_sem.at[k],
            device_id=(ta, side * p.half + ts),
            device_id_type=MESH,
        )

    def own_f(buf, k, came_from):
        t = a * p.half + seat
        return pltpu.make_async_copy(
            buf.at[k, pl.ds(t * p.wide, p.wide)], xf_buf.at[a, k, came_from], rf_sem.at[k]
        )

    def add_q(table, x, first, rows, stride, gap):
        x_high, x_low = split(x)
        y = dot(table[...], jnp.concatenate([x_high, x_high, x_low], axis=0))
        for j in range(2):
            cols = slice(j * LANES, (j + 1) * LANES)
            where = pl.ds(first + j * gap, rows, stride=stride)
            y_buf[where, :] = y[:rows, cols] + swap(y[rows:, cols], sign)

    far_first = p.pb * p.rp_local * p.piece

    def sum_q(c):
        part = x_buf.at[:, pl.ds(c * p.kc, p.kc)]
        pltpu.make_async_copy(part, part, r1_sem.at[c]).wait()

        @pl.loop(0, (p.ka // 2) * p.kc)
        def _(i):
            pair = i // p.kc
            k = c * p.kc + i % p.kc
            x = jnp.concatenate(
                [
                    x_buf[2 * pair, k].reshape(p.pb * p.share, LANES),
                    x_buf[2 * pair + 1, k].reshape(p.pb * p.share, LANES),
                ],
                axis=1,
            )
            add_q(tq, x, 2 * pair * p.kn + k, p.rp_count * p.rows, p.ka * p.kn, p.kn)

        part = xf_buf.at[:, pl.ds(c, 1)]
        pltpu.make_async_copy(part, part, rf_sem.at[c]).wait()

        @pl.loop(0, p.ka // 2)
        def _(pair):
            x = jnp.concatenate(
                [
                    xf_buf[2 * pair, c].reshape(p.pb * p.wide, LANES),
                    xf_buf[2 * pair + 1, c].reshape(p.pb * p.wide, LANES),
                ],
                axis=1,
            )
            add_q(
                tf,
                x,
                far_first + 2 * pair * p.kb + c,
                p.rp_count * p.rows,
                p.ka * p.kb,
                p.kb,
            )

    @pl.loop(0, p.steps)
    def _(c):
        @pl.loop(c * p.kc, (c + 1) * p.kc)
        def _(k):
            left_side(rot, p.kb + k, kq, (p.kb + k) * p.local_q)

        @pl.loop(0, p.devices - 1)
        def _(n):
            send_1(c, n).start()

        own_1(c).start()

        @pl.when(c + p.raw_ahead < p.kb)
        def _():
            send_0(c + p.raw_ahead).start()

        send_0(c).wait_send()
        left_side(rot, c, kq, c * p.local_q)

        @pl.loop(0, p.ka * p.half - 1)
        def _(n):
            send_f(rot, c, b, n).start()

        own_f(rot, c, b).start()
        send_0(c).wait_recv()
        left_side(far, c, kq_far, c * p.local_q)

        @pl.loop(0, p.ka * p.half - 1)
        def _(n):
            send_f(far, c, other, n).start()

        own_f(far, c, other).start()

        @pl.when(c > 0)
        def _():
            sum_q(c - 1)

    sum_q(p.steps - 1)

    def send_2(j, o):
        t = xor(b, o, p.pb)
        return pltpu.make_async_remote_copy(
            src_ref=y_buf.at[pl.ds((t * p.rp_local + j) * p.piece, p.piece)],
            dst_ref=z_buf.at[j, b],
            send_sem=s2_sem.at[j],
            recv_sem=r2_sem.at[j],
            device_id=(a, t),
            device_id_type=MESH,
        )

    def send_2f(j, o):
        t = xor(seat, o, p.half)
        return pltpu.make_async_remote_copy(
            src_ref=y_buf.at[pl.ds(((p.pb + t) * p.rp_local + j) * p.piece, p.piece)],
            dst_ref=z_buf.at[j, p.pb + seat],
            send_sem=s2_sem.at[j],
            recv_sem=r2_sem.at[j],
            device_id=(a, side * p.half + t),
            device_id_type=MESH,
        )

    def start_2(j):
        @pl.loop(1, p.pb)
        def _(o):
            send_2(j, o).start()

        @pl.loop(1, p.half)
        def _(o):
            send_2f(j, o).start()

        for mine in (b, p.pb + seat):
            pltpu.make_async_copy(
                y_buf.at[pl.ds((mine * p.rp_local + j) * p.piece, p.piece)],
                z_buf.at[j, mine],
                r2_sem.at[j],
            ).start()

    for j in range(p.ahead):
        start_2(j)

    def send_3(j, o):
        t = (a + o) % p.ka
        slot = j % p.slots
        return pltpu.make_async_remote_copy(
            src_ref=w_buf.at[slot, t],
            dst_ref=out.at[j, a],
            send_sem=s3_sem.at[slot],
            recv_sem=r3_sem.at[j],
            device_id=(t, b),
            device_id_type=MESH,
        )

    def own_3(j):
        slot = j % p.slots
        return pltpu.make_async_copy(w_buf.at[slot, a], out.at[j, a], g_sem.at[slot])

    def free_3(j):
        slot = j % p.slots
        sent = w_buf.at[slot, pl.ds(0, p.ka - 1)]
        pltpu.make_async_copy(sent, sent, s3_sem.at[slot]).wait()
        own_3(j).wait()

    near, less = p.ka * p.kn, p.ka * p.kb

    @pl.loop(0, p.rp_local)
    def _(j):
        pltpu.make_async_copy(z_buf.at[j], z_buf.at[j], r2_sem.at[j]).wait()
        slot = j % p.slots

        @pl.when(j + p.ahead < p.rp_local)
        def _():
            start_2(j + p.ahead)

        @pl.when(j >= p.slots)
        def _():
            free_3(j - p.slots)

        @pl.loop(0, p.pb)
        def _(source):
            for r in range(0, p.rows, 2):
                z = jnp.concatenate(
                    [
                        jnp.concatenate(
                            [
                                z_buf[j, source, (r + s) * near : (r + s + 1) * near, :],
                                z_buf[
                                    j,
                                    p.pb + source // 2,
                                    pl.ds((source % 2 * p.rows + r + s) * less, less),
                                    :,
                                ],
                            ],
                            axis=0,
                        )
                        for s in range(2)
                    ],
                    axis=1,
                )
                z_high, z_low = split(z)
                w = dot(tk[...], jnp.concatenate([z_high, z_high, z_low], axis=0))
                for s in range(2):
                    cols = slice(s * LANES, (s + 1) * LANES)
                    full = w[: p.re_count, cols] + swap(w[p.re_count :, cols], sign)
                    where = pl.ds(source * p.rows + r + s, p.re_local, stride=p.width)
                    for t in range(p.ka):
                        w_buf[slot, t, where, :] = full[t * p.re_local : (t + 1) * p.re_local]

        @pl.loop(1, p.ka)
        def _(o):
            send_3(j, o).start()

        own_3(j).start()

    for j in range(p.rp_local - p.slots, p.rp_local):
        free_3(j)

    @pl.loop(0, p.rp_local)
    def _(j):
        into = out.at[j, pl.ds(0, p.ka - 1)]
        pltpu.make_async_copy(into, into, r3_sem.at[j]).wait()
        sent = z_buf.at[j, pl.ds(0, p.sources - 2)]
        pltpu.make_async_copy(sent, sent, s2_sem.at[j]).wait()

    @pl.loop(0, p.steps)
    def _(c):
        sent = rot.at[pl.ds(c * p.kc, p.kc), pl.ds(0, (p.devices - 1) * p.share)]
        pltpu.make_async_copy(sent, sent, s1_sem.at[c]).wait()
        sent = rot.at[pl.ds(c, 2), pl.ds(0, (p.ka * p.half - 1) * p.wide)]
        pltpu.make_async_copy(sent, sent, sf_sem.at[c]).wait()

    for i in range(1, p.ka):
        send_v(i).wait_send()
        pass_v(i).wait_send()


def unpack(p, step, x_ref, o_ref):
    for t in range(p.ka):
        x = x_ref[0, t].reshape(step, 1, p.width, LANES)
        o_ref[0, :, :, t * p.width : (t + 1) * p.width, :] = x[..., : p.bands]
        o_ref[1, :, :, t * p.width : (t + 1) * p.width, :] = x[..., p.bands :]


def three_parts(table):
    high = lax.reduce_precision(table, 8, 7)
    low = lax.reduce_precision(table - high, 8, 7)
    return jnp.concatenate([high, low, high], axis=1).astype(jnp.bfloat16)


def local_fused(p, bloch, gauge, kq_index, qpoint, re_vectors, re_weight, rp_vectors, rp_weight):
    real, imag = gauge[0], gauge[1]
    v_in = jnp.concatenate([jnp.swapaxes(real, 1, 2), jnp.swapaxes(imag, 1, 2)], axis=2)
    right = jnp.concatenate(
        [jnp.concatenate([real, imag], axis=2), jnp.concatenate([-imag, real], axis=2)], axis=1
    )
    a, b = lax.axis_index("ka"), lax.axis_index("pb")
    slots = qpoint.reshape(p.pb, p.local_q)
    other = (b + p.half) % p.pb
    far_q = lax.dynamic_index_in_dim(slots, other, 0, keepdims=True)
    far_k = (a * p.local_k + jnp.arange(p.kb, dtype=jnp.int32))[:, None]
    first = (far_k // (MK2 * MK3) + far_q // (MK2 * MK3)) % MK1
    second = (far_k // MK3 % MK2 + far_q // MK3 % MK2) % MK2
    third = (far_k % MK3 + far_q % MK3) % MK3
    kq_far = (first * MK2 + second) * MK3 + third

    def q_table(vectors, weight, rows):
        vectors = jnp.repeat(vectors, rows, axis=0)
        points = jnp.broadcast_to(slots[:, None, :], (p.pb, rows, p.local_q)).reshape(-1)
        cosine, sine = mesh_phase(vectors, points, p.q_count)
        row = jnp.arange(vectors.shape[0], dtype=jnp.int32) % rows
        col = jnp.arange(points.shape[0], dtype=jnp.int32) // p.local_q % rows
        weight = jnp.repeat(weight, rows).astype(jnp.float32)[:, None]
        same = row[:, None] == col[None, :]
        return three_parts(
            jnp.where(
                jnp.concatenate([same, same], axis=0),
                jnp.concatenate([cosine / weight, sine / weight], axis=0),
                0.0,
            )
        )

    tq = q_table(rp_vectors, rp_weight, p.rows)
    near = p.rp_count // 2
    start = b // p.half * near
    tf = q_table(
        lax.dynamic_slice_in_dim(rp_vectors, start, near),
        lax.dynamic_slice_in_dim(rp_weight, start, near),
        2 * p.rows,
    )
    points = jnp.arange(p.k_count, dtype=jnp.int32).reshape(p.ka, p.local_k)
    points = jnp.concatenate([points[:, p.kb :].reshape(-1), points[:, : p.kb].reshape(-1)])
    cosine, sine = mesh_phase(re_vectors, points, p.k_count)
    weight = re_weight.astype(jnp.float32)[:, None]
    tk = three_parts(jnp.concatenate([cosine / weight, sine / weight], axis=0))

    f32 = jnp.float32
    dma = pltpu.SemaphoreType.DMA
    vmem = pl.BlockSpec(memory_space=pltpu.VMEM)
    any_space = pl.BlockSpec(memory_space=pl.ANY)
    smem = pl.BlockSpec(memory_space=pltpu.SMEM)
    landed = pl.pallas_call(
        functools.partial(kernel, p),
        out_shape=jax.ShapeDtypeStruct((p.rp_local, p.ka, p.block, LANES), f32),
        in_specs=[any_space, any_space, vmem, smem, smem, vmem, vmem, vmem],
        out_specs=any_space,
        scratch_shapes=[
            pltpu.VMEM((p.g_slots, 2, p.local_q, p.bands, p.bands), f32),
            pltpu.VMEM((p.k_count, p.bands, LANES), f32),
            pltpu.VMEM((p.local_k, p.devices * p.share, LANES), f32),
            pltpu.VMEM((p.kb, p.devices * p.share, LANES), f32),
            pltpu.VMEM((p.ka, p.kn, p.pb, p.share, LANES), f32),
            pltpu.VMEM((p.ka, p.kb, p.pb, p.wide, LANES), f32),
            pltpu.VMEM((p.sources * p.rp_local * p.piece, LANES), f32),
            pltpu.VMEM((p.rp_local, p.sources, p.piece, LANES), f32),
            pltpu.VMEM((p.slots, p.ka, p.block, LANES), f32),
            dma((max(p.g_slots, p.slots),)),
            dma,
            dma((p.ka,)),
            dma((p.ka,)),
            dma((p.ka,)),
            dma((p.ka,)),
            dma((p.kb,)),
            dma((p.kb,)),
            dma((p.steps,)),
            dma((p.steps,)),
            dma((p.kb,)),
            dma((p.kb,)),
            dma((p.rp_local,)),
            dma((p.rp_local,)),
            dma((p.slots,)),
            dma((p.rp_local,)),
        ],
        compiler_params=pltpu.CompilerParams(
            collective_id=0, has_side_effects=True, vmem_limit_bytes=VMEM_BYTES
        ),
    )(bloch, v_in, right, kq_index.reshape(-1), kq_far.reshape(-1), tq, tf, tk)

    step = p.re_local
    return pl.pallas_call(
        functools.partial(unpack, p, step),
        grid=(p.re_local // step, p.rp_local),
        out_shape=jax.ShapeDtypeStruct((2, p.re_local, p.rp_local, p.bands, p.bands), f32),
        in_specs=[
            pl.BlockSpec(
                (1, p.ka, step * p.width, LANES), lambda i, j: (j, 0, i, 0)
            )
        ],
        out_specs=pl.BlockSpec(
            (2, step, 1, p.bands, p.bands), lambda i, j: (0, i, j, 0, 0)
        ),
    )(landed)


def local(bloch_elements, gauge, kq_index, qpoint, re_vectors, re_weight, rp_vectors, rp_weight):
    p = Plan(
        lax.axis_size("ka"),
        lax.axis_size("pb"),
        bloch_elements.shape[1],
        bloch_elements.shape[2],
        bloch_elements.shape[3],
        re_vectors.shape[0],
        rp_vectors.shape[0],
    )
    program = functools.partial(local_fused, p) if p.fits else local_general
    return program(
        bloch_elements, gauge, kq_index, qpoint, re_vectors, re_weight, rp_vectors, rp_weight
    )


def solution(mesh):
    placed = (
        P(None, "ka", "pb", None, None),
        P(None, "ka", None, None),
        P("ka", "pb"),
        P(),
        P(),
        P(),
        P(),
        P(),
    )
    return jax.shard_map(
        local,
        mesh=mesh,
        in_specs=placed,
        out_specs=P(None, "ka", "pb", None, None),
        check_vma=False,
    )
```

```python
import functools
import math

import jax
import jax.numpy as jnp
from jax import lax
from jax.experimental import pallas as pl
from jax.experimental.pallas import tpu as pltpu
from jax.sharding import PartitionSpec as P

MK1 = 4
MK2 = 6
MK3 = 4
LANES = 128
VMEM_BYTES = 67_000_000
MESH = pl.DeviceIdType.MESH


def mesh_phase(vectors, points, total_count):
    first_index = points // (MK2 * MK3)
    second_index = points // MK3 % MK2
    third_index = points % MK3
    phase_turns = (
        vectors[:, 0:1] * (first_index * (MK2 * MK3))[None, :]
        + vectors[:, 1:2] * (second_index * (MK1 * MK3))[None, :]
        + vectors[:, 2:3] * (third_index * (MK1 * MK2))[None, :]
    )
    phase_turns = jnp.mod(phase_turns, MK1 * MK2 * MK3)
    angles = phase_turns.astype(jnp.float32) * (2.0 * math.pi / (MK1 * MK2 * MK3))
    return (jnp.cos(angles) / total_count, jnp.sin(angles) / total_count)


def rotate_gauge(elements, left_side, right_side):
    exact_mode = lax.Precision.HIGH
    real_part = jnp.matmul(elements[0], right_side[0], precision=exact_mode) - jnp.matmul(
        elements[1], right_side[1], precision=exact_mode
    )
    imag_part = jnp.matmul(elements[0], right_side[1], precision=exact_mode) + jnp.matmul(
        elements[1], right_side[0], precision=exact_mode
    )
    left_real = jnp.swapaxes(left_side[0], -1, -2)
    left_imag = jnp.swapaxes(left_side[1], -1, -2)
    rot_real = jnp.matmul(left_real, real_part, precision=exact_mode) + jnp.matmul(
        left_imag, imag_part, precision=exact_mode
    )
    rot_imag = jnp.matmul(left_real, imag_part, precision=exact_mode) - jnp.matmul(
        left_imag, real_part, precision=exact_mode
    )
    return jnp.stack([rot_real, rot_imag])


def complex_table(table, count):
    cosine, sine_table = table
    real_rows = jnp.stack([cosine, sine_table], axis=1)
    imag_rows = jnp.stack([-sine_table, cosine], axis=1)
    scale = count.astype(jnp.float32)[None, :, None, None]
    return jnp.stack([real_rows, imag_rows]) / scale


def local_general(bloch_elements, gauge, kq_index, qpoint, re_vectors, re_weight, rp_vectors, rp_weight):
    local_k = bloch_elements.shape[1]
    local_q = bloch_elements.shape[2]
    bands = bloch_elements.shape[3]
    pairs = bands * bands
    gathered = lax.all_gather(gauge, "ka", axis=1, tiled=True)
    left_side = jnp.take(gathered, kq_index, axis=1)
    rotated = rotate_gauge(bloch_elements, left_side, gauge[:, :, None])
    rotated = rotated.reshape(2, local_k, local_q, pairs)
    k_count = gathered.shape[1]
    q_count = qpoint.shape[0]
    k_table = mesh_phase(re_vectors, jnp.arange(k_count, dtype=jnp.int32), k_count)
    q_table = mesh_phase(rp_vectors, qpoint, q_count)
    ka_count = lax.axis_size("ka")
    pb_count = lax.axis_size("pb")
    re_local = re_vectors.shape[0] // ka_count
    rp_local = rp_vectors.shape[0] // pb_count
    devices = ka_count * pb_count
    column_width = pairs // devices
    leaving = rotated.reshape(2, local_k, local_q, devices, column_width).transpose(3, 0, 1, 2, 4)
    leaving = leaving.reshape(devices, 2 * local_k * local_q, column_width)
    joined = lax.all_to_all(leaving, ("ka", "pb"), split_axis=0, concat_axis=0, tiled=True)
    joined = joined.reshape(ka_count, pb_count, 2, local_k, local_q, column_width)
    k_blocks = complex_table(k_table, re_weight).reshape(
        2, ka_count, re_local, 2, ka_count, local_k
    )
    q_blocks = complex_table(q_table, rp_weight).reshape(
        2, pb_count, rp_local, 2, pb_count, local_q
    )
    exact_mode = lax.Precision.HIGH
    electron = jnp.einsum("dauemk,mpeklx->dauplx", k_blocks, joined, precision=exact_mode)
    spread = jnp.einsum("fbvdpl,dauplx->abfuvx", q_blocks, electron, precision=exact_mode)
    spread = spread.reshape(devices, 2 * re_local * rp_local, column_width)
    result = lax.all_to_all(spread, ("ka", "pb"), split_axis=0, concat_axis=0, tiled=True)
    result = result.reshape(devices, 2, re_local, rp_local, column_width)
    return result.transpose(1, 2, 3, 0, 4).reshape(2, re_local, rp_local, bands, bands)


def split(x):
    high = x.astype(jnp.bfloat16)
    low = (x - high.astype(jnp.float32)).astype(jnp.bfloat16)
    return high, low


def dot(a, b):
    return jnp.dot(a, b, preferred_element_type=jnp.float32)


def swap(x, sign):
    return pltpu.roll(x, x.shape[-1] // 2, x.ndim - 1) * sign


class Plan:
    def __init__(self, ka, pb, local_k, local_q, bands, re_count, rp_count):
        self.ka, self.pb, self.half = ka, pb, pb // 2
        self.devices = ka * pb
        self.local_k, self.local_q, self.bands = local_k, local_q, bands
        self.k_count, self.q_count = ka * local_k, pb * local_q
        self.re_count, self.rp_count = re_count, rp_count
        self.re_local, self.rp_local = re_count // ka, rp_count // pb
        self.fits = (
            2 * bands == LANES
            and bands % self.devices == 0
            and pb & (pb - 1) == 0
            and pb > 2
            and ka % 2 == 0
            and local_k % 6 == 0
        )
        if not self.fits:
            return
        self.kb = local_k // 3
        self.kn = local_k - self.kb
        self.rows = bands // self.devices
        self.share = self.rows * local_q
        self.wide = 2 * self.share
        self.width = self.rows * pb
        self.piece = self.rows * ka * self.kn
        self.sources = pb + self.half
        self.block = self.re_local * self.width
        self.raw_ahead = min(3, self.kb)
        self.g_slots = 3
        self.slots = 2
        self.ahead = 2
        self.fits = (
            self.share % 8 == 0
            and self.k_count % 16 == 0
            and self.kb % 2 == 0
            and (ka * self.kb) % 8 == 0
            and (pb * self.share) % 16 == 0
            and self.width % 8 == 0
            and self.rp_local > self.slots
        )


def digits(point):
    return point // (MK2 * MK3), point // MK3 % MK2, point % MK3


def phases(columns, points, count):
    first, second, third = (d.astype(jnp.float32) for d in digits(points))
    total = MK1 * MK2 * MK3
    turns = (
        columns[:, 0:1] * (first * (MK2 * MK3))
        + columns[:, 1:2] * (second * (MK1 * MK3))
        + columns[:, 2:3] * (third * (MK1 * MK2))
    )
    turns = turns - total * jnp.floor((turns + 0.5) / total)
    angles = turns * (2.0 * math.pi / total)
    weight = columns[:, 3:4]
    return jnp.cos(angles) / count / weight, jnp.sin(angles) / count / weight


def pick(rows, values):
    source = lax.broadcasted_iota(jnp.int32, (rows.shape[0], values.shape[1]), 1)
    chosen = jnp.where(rows == source, 1.0, 0.0).astype(jnp.bfloat16)
    return lax.dot_general(
        chosen,
        values.astype(jnp.bfloat16),
        (((1,), (1,)), ((), ())),
        preferred_element_type=jnp.float32,
    )


def put_table(table, real, imag):
    full = jnp.concatenate([real, imag], axis=0)
    high, low = split(full)
    high = high.astype(jnp.float32)
    full = jnp.concatenate([high, low.astype(jnp.float32), high], axis=1)
    table[...] = full.astype(jnp.bfloat16)


def make_tables(p, side, slots, vectors, weights, tq, tf, tk):
    f32 = jnp.float32
    iota = lambda shape, dim: lax.broadcasted_iota(jnp.int32, shape, dim)
    rp = jnp.concatenate([vectors[3:6], weights[1:2]], axis=0).astype(f32)
    re = jnp.concatenate([vectors[0:3], weights[0:1]], axis=0).astype(f32)

    def q_table(table, start, count, rows):
        row = iota((count * rows, 1), 0)
        columns = pick(start + row // rows, rp)
        width = rows * p.q_count
        col = iota((1, width), 1)
        slot = col // (rows * p.local_q) * p.local_q + col % p.local_q
        chosen = jnp.where(iota((p.q_count, width), 0) == slot, 1.0, 0.0)
        held = jnp.broadcast_to(slots[...], (8, p.q_count)).astype(f32)
        points = dot(held.astype(jnp.bfloat16), chosen.astype(jnp.bfloat16))[0:1]
        cosine, sine = phases(columns, points.astype(jnp.int32), p.q_count)
        same = row % rows == col // p.local_q % rows
        put_table(table, jnp.where(same, cosine, 0.0), jnp.where(same, sine, 0.0))

    q_table(tq, 0, p.rp_count, p.rows)
    q_table(tf, side * (p.rp_count // 2), p.rp_count // 2, 2 * p.rows)

    columns = pick(iota((p.re_count, 1), 0), re)
    col = iota((1, p.k_count), 1)
    near = p.ka * p.kn
    point = jnp.where(
        col < near,
        col // p.kn * p.local_k + p.kb + col % p.kn,
        (col - near) // p.kb * p.local_k + (col - near) % p.kb,
    )
    cosine, sine = phases(columns, point, p.k_count)
    put_table(tk, cosine, sine)


def kernel(
    p,
    bloch,
    gauge,
    qpoint,
    slots,
    vectors,
    weights,
    out,
    tq,
    tf,
    tk,
    gbuf,
    vg,
    rot,
    far,
    x_buf,
    xf_buf,
    y_buf,
    z_buf,
    w_buf,
    g_sem,
    vs_sem,
    v1_sem,
    f_sem,
    v2_sem,
    s0_sem,
    r0_sem,
    s1_sem,
    r1_sem,
    sf_sem,
    rf_sem,
    s2_sem,
    r2_sem,
    s3_sem,
    r3_sem,
):
    a = lax.axis_index("ka")
    b = lax.axis_index("pb")
    core = b % 2
    sibling = b + 1 - 2 * core
    side = b // p.half
    seat = b % p.half
    other = seat + (1 - side) * p.half
    middle = p.local_k // 2
    lane = lax.broadcasted_iota(jnp.int32, (1, LANES), 1)
    sign = jnp.where(lane < p.bands, 1.0, -1.0).astype(jnp.float32)

    def xor(x, o, count):
        t, bit = 0, 1
        while bit < count:
            t = t + (x // bit + o // bit) % 2 * bit
            bit *= 2
        return t

    def load_g(k):
        slot = k % p.g_slots
        return pltpu.make_async_copy(bloch.at[:, k], gbuf.at[slot], g_sem.at[slot])

    for k in range(p.g_slots):
        load_g(k).start()

    barrier = pltpu.get_barrier_semaphore()
    me = a * p.pb + b

    @pl.loop(1, p.devices)
    def _(o):
        t = (me + o) % p.devices
        pl.semaphore_signal(barrier, inc=1, device_id=(t // p.pb, t % p.pb), device_id_type=MESH)

    @pl.loop(0, p.local_k)
    def _(k):
        vg[a * p.local_k + k] = jnp.concatenate(
            [jnp.transpose(gauge[0, k]), jnp.transpose(gauge[1, k])], axis=1
        )

    pl.semaphore_wait(barrier, p.devices - 1)

    def send_v(i):
        return pltpu.make_async_remote_copy(
            src_ref=vg.at[pl.ds(a * p.local_k + core * middle, middle)],
            dst_ref=vg.at[pl.ds(a * p.local_k + core * middle, middle)],
            send_sem=vs_sem.at[i],
            recv_sem=v1_sem.at[i],
            device_id=((a + i) % p.ka, b),
            device_id_type=MESH,
        )

    def pass_v(i):
        source = (a + p.ka - i) % p.ka
        part = pl.ds(source * p.local_k + core * middle, middle)
        return pltpu.make_async_remote_copy(
            src_ref=vg.at[part],
            dst_ref=vg.at[part],
            send_sem=f_sem.at[i],
            recv_sem=v2_sem.at[i],
            device_id=(a, sibling),
            device_id_type=MESH,
        )

    for i in range(1, p.ka):
        send_v(i).start()

    def right_side(k, carry):
        load_g(k).wait()
        g = gbuf[k % p.g_slots]
        g = jnp.concatenate([g[0], g[1]], axis=-1).reshape(p.local_q * p.bands, LANES)
        g_high, g_low = split(g)
        u, v = gauge[0, k], gauge[1, k]
        r_high, r_low = split(
            jnp.concatenate(
                [jnp.concatenate([u, v], axis=1), jnp.concatenate([-v, u], axis=1)], axis=0
            )
        )
        h = dot(
            jnp.concatenate([g_high, g_low], axis=1), jnp.concatenate([r_high, r_high], axis=0)
        ) + dot(g_high, r_low)
        h = h.reshape(p.local_q, p.bands, LANES)
        for q in range(p.local_q):
            rot[k, pl.ds(q, p.bands, stride=p.local_q), :] = h[q]

        @pl.when(k + p.g_slots < p.local_k)
        def _():
            load_g(k + p.g_slots).start()

        return carry

    def send_0(k):
        return pltpu.make_async_remote_copy(
            src_ref=rot.at[k],
            dst_ref=far.at[k],
            send_sem=s0_sem.at[k],
            recv_sem=r0_sem.at[k],
            device_id=(a, other),
            device_id_type=MESH,
        )

    @pl.loop(0, p.raw_ahead)
    def _(k):
        right_side(k, 0)
        send_0(k).start()

    lax.fori_loop(p.raw_ahead, middle, right_side, 0)
    make_tables(p, side, slots, vectors, weights, tq, tf, tk)
    for i in range(1, p.ka):
        send_v(i).wait_recv()
        pass_v(i).start()
    lax.fori_loop(middle, p.local_k, right_side, 0)
    for i in range(1, p.ka):
        pass_v(i).wait_recv()

    def left_side(buf, row, k, source):
        k1, k2, k3 = digits(a * p.local_k + k)
        for q in range(p.local_q):
            q1, q2, q3 = digits(qpoint[source * p.local_q + q])
            kq = ((k1 + q1) % MK1 * MK2 + (k2 + q2) % MK2) * MK3 + (k3 + q3) % MK3
            v_high, v_low = split(vg[kq])
            h = buf[row, pl.ds(q, p.bands, stride=p.local_q), :]
            h_high, h_low = split(jnp.concatenate([h, swap(h, sign)], axis=0))
            buf[row, pl.ds(q, p.bands, stride=p.local_q), :] = dot(
                jnp.concatenate([v_high, v_low], axis=1),
                jnp.concatenate([h_high, h_high], axis=0),
            ) + dot(v_high, h_low)

    def send_1(c, n):
        ta = (a + p.ka - 1 - n % p.ka) % p.ka
        tb = xor(b, p.pb - 1 - n // p.ka, p.pb)
        t = ta * p.pb + tb
        return pltpu.make_async_remote_copy(
            src_ref=rot.at[p.kb + c, pl.ds(t * p.share, p.share)],
            dst_ref=x_buf.at[a, c, b],
            send_sem=s1_sem.at[c],
            recv_sem=r1_sem.at[c],
            device_id=(ta, tb),
            device_id_type=MESH,
        )

    def own_1(c):
        return pltpu.make_async_copy(
            rot.at[p.kb + c, pl.ds(me * p.share, p.share)], x_buf.at[a, c, b], r1_sem.at[c]
        )

    def send_f(buf, k, came_from, n):
        ta = (a + p.ka - 1 - n % p.ka) % p.ka
        ts = xor(seat, p.half - 1 - n // p.ka, p.half)
        t = ta * p.half + ts
        return pltpu.make_async_remote_copy(
            src_ref=buf.at[k, pl.ds(t * p.wide, p.wide)],
            dst_ref=xf_buf.at[a, k, came_from],
            send_sem=sf_sem.at[k],
            recv_sem=rf_sem.at[k],
            device_id=(ta, side * p.half + ts),
            device_id_type=MESH,
        )

    def own_f(buf, k, came_from):
        t = a * p.half + seat
        return pltpu.make_async_copy(
            buf.at[k, pl.ds(t * p.wide, p.wide)], xf_buf.at[a, k, came_from], rf_sem.at[k]
        )

    def add_q(table, x, first, rows, stride, gap):
        x_high, x_low = split(x)
        y = dot(table[...], jnp.concatenate([x_high, x_high, x_low], axis=0))
        for j in range(2):
            cols = slice(j * LANES, (j + 1) * LANES)
            where = pl.ds(first + j * gap, rows, stride=stride)
            y_buf[where, :] = y[:rows, cols] + swap(y[rows:, cols], sign)

    far_first = p.pb * p.rp_local * p.piece

    def sum_near(c):
        part = x_buf.at[:, pl.ds(c, 1)]
        pltpu.make_async_copy(part, part, r1_sem.at[c]).wait()

        @pl.loop(0, p.ka // 2)
        def _(pair):
            x = jnp.concatenate(
                [
                    x_buf[2 * pair, c].reshape(p.pb * p.share, LANES),
                    x_buf[2 * pair + 1, c].reshape(p.pb * p.share, LANES),
                ],
                axis=1,
            )
            add_q(tq, x, 2 * pair * p.kn + c, p.rp_count * p.rows, p.ka * p.kn, p.kn)

    def sum_far(c):
        part = xf_buf.at[:, pl.ds(c, 1)]
        pltpu.make_async_copy(part, part, rf_sem.at[c]).wait()

        @pl.loop(0, p.ka // 2)
        def _(pair):
            x = jnp.concatenate(
                [
                    xf_buf[2 * pair, c].reshape(p.pb * p.wide, LANES),
                    xf_buf[2 * pair + 1, c].reshape(p.pb * p.wide, LANES),
                ],
                axis=1,
            )
            add_q(
                tf,
                x,
                far_first + 2 * pair * p.kb + c,
                p.rp_count * p.rows,
                p.ka * p.kb,
                p.kb,
            )

    def begin(c):
        return c * c * p.kn // (p.kb * p.kb)

    @pl.loop(0, p.kb + 1)
    def _(c):
        @pl.when(c < p.kb)
        def _():
            send_0(c).wait_send()
            left_side(rot, c, c, b)

            @pl.loop(0, p.ka * p.half - 1)
            def _(n):
                send_f(rot, c, b, n).start()

            own_f(rot, c, b).start()
            send_0(c).wait_recv()
            left_side(far, c, c, other)

            @pl.loop(0, p.ka * p.half - 1)
            def _(n):
                send_f(far, c, other, n).start()

            own_f(far, c, other).start()

            @pl.loop(begin(c), begin(c + 1))
            def _(k):
                left_side(rot, p.kb + k, p.kb + k, b)

                @pl.loop(0, p.devices - 1)
                def _(n):
                    send_1(k, n).start()

                own_1(k).start()

            @pl.when(c + p.raw_ahead < p.kb)
            def _():
                send_0(c + p.raw_ahead).start()

        @pl.when(c > 0)
        def _():
            sum_far(c - 1)
            pl.loop(begin(c - 1), begin(c))(sum_near)

    def send_2(j, o):
        t = xor(b, o, p.pb)
        return pltpu.make_async_remote_copy(
            src_ref=y_buf.at[pl.ds((t * p.rp_local + j) * p.piece, p.piece)],
            dst_ref=z_buf.at[j, b],
            send_sem=s2_sem.at[j],
            recv_sem=r2_sem.at[j],
            device_id=(a, t),
            device_id_type=MESH,
        )

    def send_2f(j, o):
        t = xor(seat, o, p.half)
        return pltpu.make_async_remote_copy(
            src_ref=y_buf.at[pl.ds(((p.pb + t) * p.rp_local + j) * p.piece, p.piece)],
            dst_ref=z_buf.at[j, p.pb + seat],
            send_sem=s2_sem.at[j],
            recv_sem=r2_sem.at[j],
            device_id=(a, side * p.half + t),
            device_id_type=MESH,
        )

    def start_2(j):
        @pl.loop(1, p.pb)
        def _(o):
            send_2(j, o).start()

        @pl.loop(1, p.half)
        def _(o):
            send_2f(j, o).start()

        for mine in (b, p.pb + seat):
            pltpu.make_async_copy(
                y_buf.at[pl.ds((mine * p.rp_local + j) * p.piece, p.piece)],
                z_buf.at[j, mine],
                r2_sem.at[j],
            ).start()

    for j in range(p.ahead):
        start_2(j)

    def send_3(j, o):
        t = (a + o) % p.ka
        slot = j % p.slots
        return pltpu.make_async_remote_copy(
            src_ref=w_buf.at[slot, t],
            dst_ref=out.at[j, a],
            send_sem=s3_sem.at[slot],
            recv_sem=r3_sem.at[j],
            device_id=(t, b),
            device_id_type=MESH,
        )

    def own_3(j):
        slot = j % p.slots
        return pltpu.make_async_copy(w_buf.at[slot, a], out.at[j, a], g_sem.at[slot])

    def free_3(j):
        slot = j % p.slots
        sent = w_buf.at[slot, pl.ds(0, p.ka - 1)]
        pltpu.make_async_copy(sent, sent, s3_sem.at[slot]).wait()
        own_3(j).wait()

    near, less = p.ka * p.kn, p.ka * p.kb

    @pl.loop(0, p.rp_local)
    def _(j):
        pltpu.make_async_copy(z_buf.at[j], z_buf.at[j], r2_sem.at[j]).wait()
        slot = j % p.slots

        @pl.when(j + p.ahead < p.rp_local)
        def _():
            start_2(j + p.ahead)

        @pl.when(j >= p.slots)
        def _():
            free_3(j - p.slots)

        @pl.loop(0, p.pb)
        def _(source):
            for r in range(0, p.rows, 2):
                z = jnp.concatenate(
                    [
                        jnp.concatenate(
                            [
                                z_buf[j, source, (r + s) * near : (r + s + 1) * near, :],
                                z_buf[
                                    j,
                                    p.pb + source // 2,
                                    pl.ds((source % 2 * p.rows + r + s) * less, less),
                                    :,
                                ],
                            ],
                            axis=0,
                        )
                        for s in range(2)
                    ],
                    axis=1,
                )
                z_high, z_low = split(z)
                w = dot(tk[...], jnp.concatenate([z_high, z_high, z_low], axis=0))
                for s in range(2):
                    cols = slice(s * LANES, (s + 1) * LANES)
                    full = w[: p.re_count, cols] + swap(w[p.re_count :, cols], sign)
                    where = pl.ds(source * p.rows + r + s, p.re_local, stride=p.width)
                    for t in range(p.ka):
                        w_buf[slot, t, where, :] = full[t * p.re_local : (t + 1) * p.re_local]

        @pl.loop(1, p.ka)
        def _(o):
            send_3(j, o).start()

        own_3(j).start()

    for j in range(p.rp_local - p.slots, p.rp_local):
        free_3(j)

    @pl.loop(0, p.rp_local)
    def _(j):
        into = out.at[j, pl.ds(0, p.ka - 1)]
        pltpu.make_async_copy(into, into, r3_sem.at[j]).wait()
        sent = z_buf.at[j, pl.ds(0, p.sources - 2)]
        pltpu.make_async_copy(sent, sent, s2_sem.at[j]).wait()

    @pl.loop(0, p.kn)
    def _(c):
        sent = rot.at[c, pl.ds(0, (p.devices - 1) * p.share)]
        pltpu.make_async_copy(sent, sent, s1_sem.at[c]).wait()

    @pl.loop(0, p.kb)
    def _(c):
        sent = rot.at[pl.ds(c, 2), pl.ds(0, (p.ka * p.half - 1) * p.wide)]
        pltpu.make_async_copy(sent, sent, sf_sem.at[c]).wait()

    for i in range(1, p.ka):
        send_v(i).wait_send()
        pass_v(i).wait_send()


def unpack(p, step, x_ref, o_ref):
    for t in range(p.ka):
        x = x_ref[0, t].reshape(step, 1, p.width, LANES)
        o_ref[0, :, :, t * p.width : (t + 1) * p.width, :] = x[..., : p.bands]
        o_ref[1, :, :, t * p.width : (t + 1) * p.width, :] = x[..., p.bands :]


def local_fused(p, bloch, gauge, _, qpoint, re_vectors, re_weight, rp_vectors, rp_weight):
    vectors = jnp.concatenate([re_vectors.T, rp_vectors.T], axis=0)
    weights = jnp.stack([re_weight, rp_weight])
    rows_q = 2 * p.rp_count * p.rows
    f32 = jnp.float32
    dma = pltpu.SemaphoreType.DMA
    vmem = pl.BlockSpec(memory_space=pltpu.VMEM)
    any_space = pl.BlockSpec(memory_space=pl.ANY)
    smem = pl.BlockSpec(memory_space=pltpu.SMEM)
    landed = pl.pallas_call(
        functools.partial(kernel, p),
        out_shape=jax.ShapeDtypeStruct((p.rp_local, p.ka, p.block, LANES), f32),
        in_specs=[any_space, vmem, smem, vmem, vmem, vmem],
        out_specs=any_space,
        scratch_shapes=[
            pltpu.VMEM((rows_q, 3 * p.rows * p.q_count), jnp.bfloat16),
            pltpu.VMEM((rows_q, 6 * p.rows * p.q_count), jnp.bfloat16),
            pltpu.VMEM((2 * p.re_count, 3 * p.k_count), jnp.bfloat16),
            pltpu.VMEM((p.g_slots, 2, p.local_q, p.bands, p.bands), f32),
            pltpu.VMEM((p.k_count, p.bands, LANES), f32),
            pltpu.VMEM((p.local_k, p.devices * p.share, LANES), f32),
            pltpu.VMEM((p.kb, p.devices * p.share, LANES), f32),
            pltpu.VMEM((p.ka, p.kn, p.pb, p.share, LANES), f32),
            pltpu.VMEM((p.ka, p.kb, p.pb, p.wide, LANES), f32),
            pltpu.VMEM((p.sources * p.rp_local * p.piece, LANES), f32),
            pltpu.VMEM((p.rp_local, p.sources, p.piece, LANES), f32),
            pltpu.VMEM((p.slots, p.ka, p.block, LANES), f32),
            dma((max(p.g_slots, p.slots),)),
            dma((p.ka,)),
            dma((p.ka,)),
            dma((p.ka,)),
            dma((p.ka,)),
            dma((p.kb,)),
            dma((p.kb,)),
            dma((p.kn,)),
            dma((p.kn,)),
            dma((p.kb,)),
            dma((p.kb,)),
            dma((p.rp_local,)),
            dma((p.rp_local,)),
            dma((p.slots,)),
            dma((p.rp_local,)),
        ],
        compiler_params=pltpu.CompilerParams(
            collective_id=0, has_side_effects=True, vmem_limit_bytes=VMEM_BYTES
        ),
    )(bloch, gauge, qpoint, qpoint.reshape(1, -1), vectors, weights)

    step = p.re_local
    return pl.pallas_call(
        functools.partial(unpack, p, step),
        grid=(p.re_local // step, p.rp_local),
        out_shape=jax.ShapeDtypeStruct((2, p.re_local, p.rp_local, p.bands, p.bands), f32),
        in_specs=[
            pl.BlockSpec(
                (1, p.ka, step * p.width, LANES), lambda i, j: (j, 0, i, 0)
            )
        ],
        out_specs=pl.BlockSpec(
            (2, step, 1, p.bands, p.bands), lambda i, j: (0, i, j, 0, 0)
        ),
    )(landed)


def local(bloch_elements, gauge, kq_index, qpoint, re_vectors, re_weight, rp_vectors, rp_weight):
    p = Plan(
        lax.axis_size("ka"),
        lax.axis_size("pb"),
        bloch_elements.shape[1],
        bloch_elements.shape[2],
        bloch_elements.shape[3],
        re_vectors.shape[0],
        rp_vectors.shape[0],
    )
    program = functools.partial(local_fused, p) if p.fits else local_general
    return program(
        bloch_elements, gauge, kq_index, qpoint, re_vectors, re_weight, rp_vectors, rp_weight
    )


def solution(mesh):
    placed = (
        P(None, "ka", "pb", None, None),
        P(None, "ka", None, None),
        P("ka", "pb"),
        P(),
        P(),
        P(),
        P(),
        P(),
    )
    return jax.shard_map(
        local,
        mesh=mesh,
        in_specs=placed,
        out_specs=P(None, "ka", "pb", None, None),
        check_vma=False,
    )
```

```python
import functools
import math

import jax
import jax.numpy as jnp
from jax import lax
from jax.experimental import pallas as pl
from jax.experimental.pallas import tpu as pltpu
from jax.sharding import PartitionSpec as P

MK1 = 4
MK2 = 6
MK3 = 4
LANES = 128
UNPACK_SLOTS = 8
VMEM_BYTES = 67_000_000
MESH = pl.DeviceIdType.MESH


def mesh_phase(vectors, points, total_count):
    first_index = points // (MK2 * MK3)
    second_index = points // MK3 % MK2
    third_index = points % MK3
    phase_turns = (
        vectors[:, 0:1] * (first_index * (MK2 * MK3))[None, :]
        + vectors[:, 1:2] * (second_index * (MK1 * MK3))[None, :]
        + vectors[:, 2:3] * (third_index * (MK1 * MK2))[None, :]
    )
    phase_turns = jnp.mod(phase_turns, MK1 * MK2 * MK3)
    angles = phase_turns.astype(jnp.float32) * (2.0 * math.pi / (MK1 * MK2 * MK3))
    return (jnp.cos(angles) / total_count, jnp.sin(angles) / total_count)


def rotate_gauge(elements, left_side, right_side):
    exact_mode = lax.Precision.HIGH
    real_part = jnp.matmul(elements[0], right_side[0], precision=exact_mode) - jnp.matmul(
        elements[1], right_side[1], precision=exact_mode
    )
    imag_part = jnp.matmul(elements[0], right_side[1], precision=exact_mode) + jnp.matmul(
        elements[1], right_side[0], precision=exact_mode
    )
    left_real = jnp.swapaxes(left_side[0], -1, -2)
    left_imag = jnp.swapaxes(left_side[1], -1, -2)
    rot_real = jnp.matmul(left_real, real_part, precision=exact_mode) + jnp.matmul(
        left_imag, imag_part, precision=exact_mode
    )
    rot_imag = jnp.matmul(left_real, imag_part, precision=exact_mode) - jnp.matmul(
        left_imag, real_part, precision=exact_mode
    )
    return jnp.stack([rot_real, rot_imag])


def complex_table(table, count):
    cosine, sine_table = table
    real_rows = jnp.stack([cosine, sine_table], axis=1)
    imag_rows = jnp.stack([-sine_table, cosine], axis=1)
    scale = count.astype(jnp.float32)[None, :, None, None]
    return jnp.stack([real_rows, imag_rows]) / scale


def local_general(bloch_elements, gauge, kq_index, qpoint, re_vectors, re_weight, rp_vectors, rp_weight):
    local_k = bloch_elements.shape[1]
    local_q = bloch_elements.shape[2]
    bands = bloch_elements.shape[3]
    pairs = bands * bands
    gathered = lax.all_gather(gauge, "ka", axis=1, tiled=True)
    left_side = jnp.take(gathered, kq_index, axis=1)
    rotated = rotate_gauge(bloch_elements, left_side, gauge[:, :, None])
    rotated = rotated.reshape(2, local_k, local_q, pairs)
    k_count = gathered.shape[1]
    q_count = qpoint.shape[0]
    k_table = mesh_phase(re_vectors, jnp.arange(k_count, dtype=jnp.int32), k_count)
    q_table = mesh_phase(rp_vectors, qpoint, q_count)
    ka_count = lax.axis_size("ka")
    pb_count = lax.axis_size("pb")
    re_local = re_vectors.shape[0] // ka_count
    rp_local = rp_vectors.shape[0] // pb_count
    devices = ka_count * pb_count
    column_width = pairs // devices
    leaving = rotated.reshape(2, local_k, local_q, devices, column_width).transpose(3, 0, 1, 2, 4)
    leaving = leaving.reshape(devices, 2 * local_k * local_q, column_width)
    joined = lax.all_to_all(leaving, ("ka", "pb"), split_axis=0, concat_axis=0, tiled=True)
    joined = joined.reshape(ka_count, pb_count, 2, local_k, local_q, column_width)
    k_blocks = complex_table(k_table, re_weight).reshape(
        2, ka_count, re_local, 2, ka_count, local_k
    )
    q_blocks = complex_table(q_table, rp_weight).reshape(
        2, pb_count, rp_local, 2, pb_count, local_q
    )
    exact_mode = lax.Precision.HIGH
    electron = jnp.einsum("dauemk,mpeklx->dauplx", k_blocks, joined, precision=exact_mode)
    spread = jnp.einsum("fbvdpl,dauplx->abfuvx", q_blocks, electron, precision=exact_mode)
    spread = spread.reshape(devices, 2 * re_local * rp_local, column_width)
    result = lax.all_to_all(spread, ("ka", "pb"), split_axis=0, concat_axis=0, tiled=True)
    result = result.reshape(devices, 2, re_local, rp_local, column_width)
    return result.transpose(1, 2, 3, 0, 4).reshape(2, re_local, rp_local, bands, bands)


def split(x):
    high = x.astype(jnp.bfloat16)
    low = (x - high.astype(jnp.float32)).astype(jnp.bfloat16)
    return high, low


def dot(a, b):
    return jnp.dot(a, b, preferred_element_type=jnp.float32)


def swap(x, sign):
    return pltpu.roll(x, x.shape[-1] // 2, x.ndim - 1) * sign


class Plan:
    def __init__(self, ka, pb, local_k, local_q, bands, re_count, rp_count):
        self.ka, self.pb, self.half = ka, pb, pb // 2
        self.devices = ka * pb
        self.local_k, self.local_q, self.bands = local_k, local_q, bands
        self.k_count, self.q_count = ka * local_k, pb * local_q
        self.re_count, self.rp_count = re_count, rp_count
        self.re_local, self.rp_local = re_count // ka, rp_count // pb
        self.fits = (
            2 * bands == LANES
            and bands % self.devices == 0
            and pb & (pb - 1) == 0
            and pb > 2
            and ka % 2 == 0
            and local_k % 6 == 0
        )
        if not self.fits:
            return
        self.kb = local_k // 3
        self.kn = local_k - self.kb
        self.rows = bands // self.devices
        self.share = self.rows * local_q
        self.wide = 2 * self.share
        self.width = self.rows * pb
        self.piece = ka * self.kn
        self.chunks = self.rp_local * self.rows
        self.sources = pb + self.half
        self.block = self.re_local * pb
        self.raw_ahead = min(3, self.kb)
        self.g_slots = 3
        self.slots = 2
        self.ahead = 4
        self.fits = (
            self.share % 8 == 0
            and self.k_count % 16 == 0
            and self.kb % 2 == 0
            and (ka * self.kb) % 8 == 0
            and (pb * self.share) % 16 == 0
            and pb % 8 == 0
            and self.chunks > self.slots
            and self.rp_local > UNPACK_SLOTS
        )


def digits(point):
    return point // (MK2 * MK3), point // MK3 % MK2, point % MK3


def phases(columns, points, count):
    first, second, third = (d.astype(jnp.float32) for d in digits(points))
    total = MK1 * MK2 * MK3
    turns = (
        columns[:, 0:1] * (first * (MK2 * MK3))
        + columns[:, 1:2] * (second * (MK1 * MK3))
        + columns[:, 2:3] * (third * (MK1 * MK2))
    )
    turns = turns - total * jnp.floor((turns + 0.5) / total)
    angles = turns * (2.0 * math.pi / total)
    weight = columns[:, 3:4]
    return jnp.cos(angles) / count / weight, jnp.sin(angles) / count / weight


def pick(rows, values):
    source = lax.broadcasted_iota(jnp.int32, (rows.shape[0], values.shape[1]), 1)
    chosen = jnp.where(rows == source, 1.0, 0.0).astype(jnp.bfloat16)
    return lax.dot_general(
        chosen,
        values.astype(jnp.bfloat16),
        (((1,), (1,)), ((), ())),
        preferred_element_type=jnp.float32,
    )


def put_table(table, real, imag):
    full = jnp.concatenate([real, imag], axis=0)
    high, low = split(full)
    high = high.astype(jnp.float32)
    full = jnp.concatenate([high, low.astype(jnp.float32), high], axis=1)
    table[...] = full.astype(jnp.bfloat16)


def make_tables(p, side, slots, re, rp, tq, tf, tk):
    f32 = jnp.float32
    iota = lambda shape, dim: lax.broadcasted_iota(jnp.int32, shape, dim)
    re, rp = re.astype(f32), rp.astype(f32)

    def q_table(table, start, count, rows, inner):
        row = iota((count * rows, 1), 0)
        band = row % rows % inner * (rows // inner) + row % rows // inner
        columns = pick(start + row // rows, rp)
        width = rows * p.q_count
        col = iota((1, width), 1)
        slot = col // (rows * p.local_q) * p.local_q + col % p.local_q
        chosen = jnp.where(iota((p.q_count, width), 0) == slot, 1.0, 0.0)
        held = jnp.broadcast_to(slots[...], (8, p.q_count)).astype(f32)
        points = dot(held.astype(jnp.bfloat16), chosen.astype(jnp.bfloat16))[0:1]
        cosine, sine = phases(columns, points.astype(jnp.int32), p.q_count)
        same = band == col // p.local_q % rows
        put_table(table, jnp.where(same, cosine, 0.0), jnp.where(same, sine, 0.0))

    q_table(tq, 0, p.rp_count, p.rows, 1)
    q_table(tf, side * (p.rp_count // 2), p.rp_count // 2, 2 * p.rows, 2)

    columns = pick(iota((p.re_count, 1), 0), re)
    col = iota((1, p.k_count), 1)
    near = p.ka * p.kn
    point = jnp.where(
        col < near,
        col // p.kn * p.local_k + p.kb + col % p.kn,
        (col - near) // p.kb * p.local_k + (col - near) % p.kb,
    )
    cosine, sine = phases(columns, point, p.k_count)
    put_table(tk, cosine, sine)


def kernel(
    p,
    bloch,
    gauge,
    qpoint,
    slots,
    re_vectors,
    re_weight,
    rp_vectors,
    rp_weight,
    out,
    tq,
    tf,
    tk,
    gbuf,
    vg,
    rot,
    far,
    x_buf,
    xf_buf,
    y_buf,
    z_buf,
    w_buf,
    g_sem,
    vs_sem,
    v1_sem,
    f_sem,
    v2_sem,
    s0_sem,
    r0_sem,
    s1_sem,
    r1_sem,
    sf_sem,
    rf_sem,
    s2_sem,
    r2_sem,
    s3_sem,
    r3_sem,
):
    a = lax.axis_index("ka")
    b = lax.axis_index("pb")
    core = b % 2
    sibling = b + 1 - 2 * core
    side = b // p.half
    seat = b % p.half
    other = seat + (1 - side) * p.half
    middle = p.local_k // 2
    lane = lax.broadcasted_iota(jnp.int32, (1, LANES), 1)
    sign = jnp.where(lane < p.bands, 1.0, -1.0).astype(jnp.float32)

    def xor(x, o, count):
        t, bit = 0, 1
        while bit < count:
            t = t + (x // bit + o // bit) % 2 * bit
            bit *= 2
        return t

    def load_g(k):
        slot = k % p.g_slots
        return pltpu.make_async_copy(bloch.at[:, k], gbuf.at[slot], g_sem.at[slot])

    for k in range(p.g_slots):
        load_g(k).start()

    barrier = pltpu.get_barrier_semaphore()
    me = a * p.pb + b

    @pl.loop(1, p.devices)
    def _(o):
        t = (me + o) % p.devices
        pl.semaphore_signal(barrier, inc=1, device_id=(t // p.pb, t % p.pb), device_id_type=MESH)

    @pl.loop(0, p.local_k)
    def _(k):
        v = jnp.concatenate([jnp.transpose(gauge[0, k]), jnp.transpose(gauge[1, k])], axis=1)
        for t in range(p.ka):
            for r in range(p.rows):
                first = t * p.width + r * p.pb
                where = pl.ds(t * p.width + r, p.pb, stride=p.rows)
                vg[a * p.local_k + k, where, :] = v[first : first + p.pb]

    pl.semaphore_wait(barrier, p.devices - 1)

    def send_v(i):
        return pltpu.make_async_remote_copy(
            src_ref=vg.at[pl.ds(a * p.local_k + core * middle, middle)],
            dst_ref=vg.at[pl.ds(a * p.local_k + core * middle, middle)],
            send_sem=vs_sem.at[i],
            recv_sem=v1_sem.at[i],
            device_id=((a + i) % p.ka, b),
            device_id_type=MESH,
        )

    def pass_v(i):
        source = (a + p.ka - i) % p.ka
        part = pl.ds(source * p.local_k + core * middle, middle)
        return pltpu.make_async_remote_copy(
            src_ref=vg.at[part],
            dst_ref=vg.at[part],
            send_sem=f_sem.at[i],
            recv_sem=v2_sem.at[i],
            device_id=(a, sibling),
            device_id_type=MESH,
        )

    for i in range(1, p.ka):
        send_v(i).start()

    def right_side(k, carry):
        load_g(k).wait()
        g = gbuf[k % p.g_slots]
        g = jnp.concatenate([g[0], g[1]], axis=-1).reshape(p.local_q * p.bands, LANES)
        g_high, g_low = split(g)
        u, v = gauge[0, k], gauge[1, k]
        r_high, r_low = split(
            jnp.concatenate(
                [jnp.concatenate([u, v], axis=1), jnp.concatenate([-v, u], axis=1)], axis=0
            )
        )
        h = dot(
            jnp.concatenate([g_high, g_low], axis=1), jnp.concatenate([r_high, r_high], axis=0)
        ) + dot(g_high, r_low)
        h = h.reshape(p.local_q, p.bands, LANES)
        for q in range(p.local_q):
            rot[k, pl.ds(q, p.bands, stride=p.local_q), :] = h[q]

        @pl.when(k + p.g_slots < p.local_k)
        def _():
            load_g(k + p.g_slots).start()

        return carry

    def send_0(k):
        return pltpu.make_async_remote_copy(
            src_ref=rot.at[k],
            dst_ref=far.at[k],
            send_sem=s0_sem.at[k],
            recv_sem=r0_sem.at[k],
            device_id=(a, other),
            device_id_type=MESH,
        )

    @pl.loop(0, p.raw_ahead)
    def _(k):
        right_side(k, 0)
        send_0(k).start()

    lax.fori_loop(p.raw_ahead, middle, right_side, 0)
    re = jnp.concatenate([re_vectors[...], re_weight[...]], axis=0)
    rp = jnp.concatenate([rp_vectors[...], rp_weight[...]], axis=0)
    make_tables(p, side, slots, re, rp, tq, tf, tk)
    for i in range(1, p.ka):
        send_v(i).wait_recv()
        pass_v(i).start()
    lax.fori_loop(middle, p.local_k, right_side, 0)
    for i in range(1, p.ka):
        pass_v(i).wait_recv()

    def left_side(buf, row, k, source):
        k1, k2, k3 = digits(a * p.local_k + k)
        for q in range(p.local_q):
            q1, q2, q3 = digits(qpoint[source * p.local_q + q])
            kq = ((k1 + q1) % MK1 * MK2 + (k2 + q2) % MK2) * MK3 + (k3 + q3) % MK3
            v_high, v_low = split(vg[kq])
            h = buf[row, pl.ds(q, p.bands, stride=p.local_q), :]
            h_high, h_low = split(jnp.concatenate([h, swap(h, sign)], axis=0))
            buf[row, pl.ds(q, p.bands, stride=p.local_q), :] = dot(
                jnp.concatenate([v_high, v_low], axis=1),
                jnp.concatenate([h_high, h_high], axis=0),
            ) + dot(v_high, h_low)

    def send_1(c, n):
        ta = (a + p.ka - 1 - n % p.ka) % p.ka
        tb = xor(b, p.pb - 1 - n // p.ka, p.pb)
        t = ta * p.pb + tb
        return pltpu.make_async_remote_copy(
            src_ref=rot.at[p.kb + c, pl.ds(t * p.share, p.share)],
            dst_ref=x_buf.at[a, c, b],
            send_sem=s1_sem.at[c],
            recv_sem=r1_sem.at[c],
            device_id=(ta, tb),
            device_id_type=MESH,
        )

    def own_1(c):
        return pltpu.make_async_copy(
            rot.at[p.kb + c, pl.ds(me * p.share, p.share)], x_buf.at[a, c, b], r1_sem.at[c]
        )

    def send_f(buf, k, came_from, n):
        ta = (a + p.ka - 1 - n % p.ka) % p.ka
        ts = xor(seat, p.half - 1 - n // p.ka, p.half)
        t = ta * p.half + ts
        return pltpu.make_async_remote_copy(
            src_ref=buf.at[k, pl.ds(t * p.wide, p.wide)],
            dst_ref=xf_buf.at[a, k, came_from],
            send_sem=sf_sem.at[k],
            recv_sem=rf_sem.at[k],
            device_id=(ta, side * p.half + ts),
            device_id_type=MESH,
        )

    def own_f(buf, k, came_from):
        t = a * p.half + seat
        return pltpu.make_async_copy(
            buf.at[k, pl.ds(t * p.wide, p.wide)], xf_buf.at[a, k, came_from], rf_sem.at[k]
        )

    def add_q(table, x, first, rows, stride, gap):
        x_high, x_low = split(x)
        y = dot(table[...], jnp.concatenate([x_high, x_high, x_low], axis=0))
        for j in range(2):
            cols = slice(j * LANES, (j + 1) * LANES)
            where = pl.ds(first + j * gap, rows, stride=stride)
            y_buf[where, :] = y[:rows, cols] + swap(y[rows:, cols], sign)

    far_first = p.pb * p.chunks * p.piece

    def sum_near(c):
        part = x_buf.at[:, pl.ds(c, 1)]
        pltpu.make_async_copy(part, part, r1_sem.at[c]).wait()

        @pl.loop(0, p.ka // 2)
        def _(pair):
            x = jnp.concatenate(
                [
                    x_buf[2 * pair, c].reshape(p.pb * p.share, LANES),
                    x_buf[2 * pair + 1, c].reshape(p.pb * p.share, LANES),
                ],
                axis=1,
            )
            add_q(tq, x, 2 * pair * p.kn + c, p.rp_count * p.rows, p.ka * p.kn, p.kn)

    def sum_far(c):
        part = xf_buf.at[:, pl.ds(c, 1)]
        pltpu.make_async_copy(part, part, rf_sem.at[c]).wait()

        @pl.loop(0, p.ka // 2)
        def _(pair):
            x = jnp.concatenate(
                [
                    xf_buf[2 * pair, c].reshape(p.pb * p.wide, LANES),
                    xf_buf[2 * pair + 1, c].reshape(p.pb * p.wide, LANES),
                ],
                axis=1,
            )
            add_q(
                tf,
                x,
                far_first + 2 * pair * p.kb + c,
                p.rp_count * p.rows,
                p.ka * p.kb,
                p.kb,
            )

    def begin(c):
        return c * c * p.kn // (p.kb * p.kb)

    @pl.loop(0, p.kb + 1)
    def _(c):
        @pl.when(c < p.kb)
        def _():
            send_0(c).wait_send()
            left_side(rot, c, c, b)

            @pl.loop(0, p.ka * p.half - 1)
            def _(n):
                send_f(rot, c, b, n).start()

            own_f(rot, c, b).start()
            send_0(c).wait_recv()
            left_side(far, c, c, other)

            @pl.loop(0, p.ka * p.half - 1)
            def _(n):
                send_f(far, c, other, n).start()

            own_f(far, c, other).start()

            @pl.loop(begin(c), begin(c + 1))
            def _(k):
                left_side(rot, p.kb + k, p.kb + k, b)

                @pl.loop(0, p.devices - 1)
                def _(n):
                    send_1(k, n).start()

                own_1(k).start()

            @pl.when(c + p.raw_ahead < p.kb)
            def _():
                send_0(c + p.raw_ahead).start()

        @pl.when(c > 0)
        def _():
            sum_far(c - 1)
            pl.loop(begin(c - 1), begin(c))(sum_near)

    def send_2(j, o):
        t = xor(b, o, p.pb)
        return pltpu.make_async_remote_copy(
            src_ref=y_buf.at[pl.ds((t * p.chunks + j) * p.piece, p.piece)],
            dst_ref=z_buf.at[j, b],
            send_sem=s2_sem.at[j],
            recv_sem=r2_sem.at[j],
            device_id=(a, t),
            device_id_type=MESH,
        )

    def send_2f(j, o):
        t = xor(seat, o, p.half)
        return pltpu.make_async_remote_copy(
            src_ref=y_buf.at[pl.ds(((p.pb + t) * p.chunks + j) * p.piece, p.piece)],
            dst_ref=z_buf.at[j, p.pb + seat],
            send_sem=s2_sem.at[j],
            recv_sem=r2_sem.at[j],
            device_id=(a, side * p.half + t),
            device_id_type=MESH,
        )

    def start_2(j):
        @pl.loop(1, p.pb)
        def _(o):
            send_2(j, o).start()

        @pl.loop(1, p.half)
        def _(o):
            send_2f(j, o).start()

        for mine in (b, p.pb + seat):
            pltpu.make_async_copy(
                y_buf.at[pl.ds((mine * p.chunks + j) * p.piece, p.piece)],
                z_buf.at[j, mine],
                r2_sem.at[j],
            ).start()

    for j in range(p.ahead):
        start_2(j)

    def send_3(j, o):
        t = (a + o) % p.ka
        slot = j % p.slots
        return pltpu.make_async_remote_copy(
            src_ref=w_buf.at[slot, t],
            dst_ref=out.at[j, a],
            send_sem=s3_sem.at[slot],
            recv_sem=r3_sem.at[j],
            device_id=(t, b),
            device_id_type=MESH,
        )

    def own_3(j):
        slot = j % p.slots
        return pltpu.make_async_copy(w_buf.at[slot, a], out.at[j, a], g_sem.at[slot])

    def free_3(j):
        slot = j % p.slots
        sent = w_buf.at[slot, pl.ds(0, p.ka - 1)]
        pltpu.make_async_copy(sent, sent, s3_sem.at[slot]).wait()
        own_3(j).wait()

    less = p.ka * p.kb

    @pl.loop(0, p.chunks)
    def _(j):
        pltpu.make_async_copy(z_buf.at[j], z_buf.at[j], r2_sem.at[j]).wait()
        slot = j % p.slots

        @pl.when(j + p.ahead < p.chunks)
        def _():
            start_2(j + p.ahead)

        @pl.when(j >= p.slots)
        def _():
            free_3(j - p.slots)

        @pl.loop(0, p.half)
        def _(s):
            far_part = z_buf[j, p.pb + s]
            z = jnp.concatenate(
                [
                    jnp.concatenate(
                        [z_buf[j, 2 * s + i], far_part[i * less : (i + 1) * less]], axis=0
                    )
                    for i in range(2)
                ],
                axis=1,
            )
            z_high, z_low = split(z)
            w = dot(tk[...], jnp.concatenate([z_high, z_high, z_low], axis=0))
            for i in range(2):
                cols = slice(i * LANES, (i + 1) * LANES)
                full = w[: p.re_count, cols] + swap(w[p.re_count :, cols], sign)
                where = pl.ds(2 * s + i, p.re_local, stride=p.pb)
                for t in range(p.ka):
                    w_buf[slot, t, where, :] = full[t * p.re_local : (t + 1) * p.re_local]

        @pl.loop(1, p.ka)
        def _(o):
            send_3(j, o).start()

        own_3(j).start()

    for j in range(p.chunks - p.slots, p.chunks):
        free_3(j)

    @pl.loop(0, p.chunks)
    def _(j):
        into = out.at[j, pl.ds(0, p.ka - 1)]
        pltpu.make_async_copy(into, into, r3_sem.at[j]).wait()
        sent = z_buf.at[j, pl.ds(0, p.sources - 2)]
        pltpu.make_async_copy(sent, sent, s2_sem.at[j]).wait()

    @pl.loop(0, p.kn)
    def _(c):
        sent = rot.at[c, pl.ds(0, (p.devices - 1) * p.share)]
        pltpu.make_async_copy(sent, sent, s1_sem.at[c]).wait()

    @pl.loop(0, p.kb)
    def _(c):
        sent = rot.at[pl.ds(c, 2), pl.ds(0, (p.ka * p.half - 1) * p.wide)]
        pltpu.make_async_copy(sent, sent, sf_sem.at[c]).wait()

    for i in range(1, p.ka):
        send_v(i).wait_send()
        pass_v(i).wait_send()


def unpack(p, x_ref, o_ref, x_buf, o_buf, x_sem, o_sem):
    def load(j):
        slot = j % UNPACK_SLOTS
        return pltpu.make_async_copy(
            x_ref.at[pl.ds(j * p.rows, p.rows)], x_buf.at[slot], x_sem.at[slot]
        )

    def store(j):
        slot = j % UNPACK_SLOTS
        return pltpu.make_async_copy(o_buf.at[slot], o_ref.at[:, :, j], o_sem.at[slot])

    for j in range(UNPACK_SLOTS):
        load(j).start()

    @pl.loop(0, p.rp_local)
    def _(j):
        slot = j % UNPACK_SLOTS
        load(j).wait()

        @pl.when(j >= UNPACK_SLOTS)
        def _():
            store(j - UNPACK_SLOTS).wait()

        for r in range(p.rows):
            for t in range(p.ka):
                x = x_buf[slot, r, t].reshape(p.re_local, p.pb, LANES)
                first = t * p.width + r * p.pb
                o_buf[slot, 0, :, first : first + p.pb, :] = x[..., : p.bands]
                o_buf[slot, 1, :, first : first + p.pb, :] = x[..., p.bands :]
        store(j).start()

        @pl.when(j + UNPACK_SLOTS < p.rp_local)
        def _():
            load(j + UNPACK_SLOTS).start()

    for j in range(p.rp_local - UNPACK_SLOTS, p.rp_local):
        store(j).wait()


def local_fused(p, bloch, gauge, _, qpoint, re_vectors, re_weight, rp_vectors, rp_weight):
    rows_q = 2 * p.rp_count * p.rows
    f32 = jnp.float32
    dma = pltpu.SemaphoreType.DMA
    vmem = pl.BlockSpec(memory_space=pltpu.VMEM)
    any_space = pl.BlockSpec(memory_space=pl.ANY)
    smem = pl.BlockSpec(memory_space=pltpu.SMEM)
    landed = pl.pallas_call(
        functools.partial(kernel, p),
        out_shape=jax.ShapeDtypeStruct((p.chunks, p.ka, p.block, LANES), f32),
        in_specs=[any_space, vmem, smem, vmem, vmem, vmem, vmem, vmem],
        out_specs=any_space,
        scratch_shapes=[
            pltpu.VMEM((rows_q, 3 * p.rows * p.q_count), jnp.bfloat16),
            pltpu.VMEM((rows_q, 6 * p.rows * p.q_count), jnp.bfloat16),
            pltpu.VMEM((2 * p.re_count, 3 * p.k_count), jnp.bfloat16),
            pltpu.VMEM((p.g_slots, 2, p.local_q, p.bands, p.bands), f32),
            pltpu.VMEM((p.k_count, p.bands, LANES), f32),
            pltpu.VMEM((p.local_k, p.devices * p.share, LANES), f32),
            pltpu.VMEM((p.kb, p.devices * p.share, LANES), f32),
            pltpu.VMEM((p.ka, p.kn, p.pb, p.share, LANES), f32),
            pltpu.VMEM((p.ka, p.kb, p.pb, p.wide, LANES), f32),
            pltpu.VMEM((p.sources * p.chunks * p.piece, LANES), f32),
            pltpu.VMEM((p.chunks, p.sources, p.piece, LANES), f32),
            pltpu.VMEM((p.slots, p.ka, p.block, LANES), f32),
            dma((max(p.g_slots, p.slots),)),
            dma((p.ka,)),
            dma((p.ka,)),
            dma((p.ka,)),
            dma((p.ka,)),
            dma((p.kb,)),
            dma((p.kb,)),
            dma((p.kn,)),
            dma((p.kn,)),
            dma((p.kb,)),
            dma((p.kb,)),
            dma((p.chunks,)),
            dma((p.chunks,)),
            dma((p.slots,)),
            dma((p.chunks,)),
        ],
        compiler_params=pltpu.CompilerParams(
            collective_id=0, has_side_effects=True, vmem_limit_bytes=VMEM_BYTES
        ),
    )(
        bloch,
        gauge,
        qpoint,
        qpoint.reshape(1, -1),
        re_vectors.T,
        re_weight.reshape(1, -1),
        rp_vectors.T,
        rp_weight.reshape(1, -1),
    )

    return pl.pallas_call(
        functools.partial(unpack, p),
        out_shape=jax.ShapeDtypeStruct((2, p.re_local, p.rp_local, p.bands, p.bands), f32),
        in_specs=[any_space],
        out_specs=any_space,
        scratch_shapes=[
            pltpu.VMEM((UNPACK_SLOTS, p.rows, p.ka, p.block, LANES), f32),
            pltpu.VMEM((UNPACK_SLOTS, 2, p.re_local, p.bands, p.bands), f32),
            dma((UNPACK_SLOTS,)),
            dma((UNPACK_SLOTS,)),
        ],
        compiler_params=pltpu.CompilerParams(vmem_limit_bytes=VMEM_BYTES),
    )(landed)


def local(bloch_elements, gauge, kq_index, qpoint, re_vectors, re_weight, rp_vectors, rp_weight):
    p = Plan(
        lax.axis_size("ka"),
        lax.axis_size("pb"),
        bloch_elements.shape[1],
        bloch_elements.shape[2],
        bloch_elements.shape[3],
        re_vectors.shape[0],
        rp_vectors.shape[0],
    )
    program = functools.partial(local_fused, p) if p.fits else local_general
    return program(
        bloch_elements, gauge, kq_index, qpoint, re_vectors, re_weight, rp_vectors, rp_weight
    )


def solution(mesh):
    placed = (
        P(None, "ka", "pb", None, None),
        P(None, "ka", None, None),
        P("ka", "pb"),
        P(),
        P(),
        P(),
        P(),
        P(),
    )
    return jax.shard_map(
        local,
        mesh=mesh,
        in_specs=placed,
        out_specs=P(None, "ka", "pb", None, None),
        check_vma=False,
    )
```

```python
import functools
import math

import jax
import jax.numpy as jnp
from jax import lax
from jax.experimental import pallas as pl
from jax.experimental.pallas import tpu as pltpu
from jax.sharding import PartitionSpec as P

MK1 = 4
MK2 = 6
MK3 = 4
LANES = 128
UNPACK_SLOTS = 8
VMEM_BYTES = 67_000_000
MESH = pl.DeviceIdType.MESH


def mesh_phase(vectors, points, total_count):
    first_index = points // (MK2 * MK3)
    second_index = points // MK3 % MK2
    third_index = points % MK3
    phase_turns = (
        vectors[:, 0:1] * (first_index * (MK2 * MK3))[None, :]
        + vectors[:, 1:2] * (second_index * (MK1 * MK3))[None, :]
        + vectors[:, 2:3] * (third_index * (MK1 * MK2))[None, :]
    )
    phase_turns = jnp.mod(phase_turns, MK1 * MK2 * MK3)
    angles = phase_turns.astype(jnp.float32) * (2.0 * math.pi / (MK1 * MK2 * MK3))
    return (jnp.cos(angles) / total_count, jnp.sin(angles) / total_count)


def rotate_gauge(elements, left_side, right_side):
    exact_mode = lax.Precision.HIGH
    real_part = jnp.matmul(elements[0], right_side[0], precision=exact_mode) - jnp.matmul(
        elements[1], right_side[1], precision=exact_mode
    )
    imag_part = jnp.matmul(elements[0], right_side[1], precision=exact_mode) + jnp.matmul(
        elements[1], right_side[0], precision=exact_mode
    )
    left_real = jnp.swapaxes(left_side[0], -1, -2)
    left_imag = jnp.swapaxes(left_side[1], -1, -2)
    rot_real = jnp.matmul(left_real, real_part, precision=exact_mode) + jnp.matmul(
        left_imag, imag_part, precision=exact_mode
    )
    rot_imag = jnp.matmul(left_real, imag_part, precision=exact_mode) - jnp.matmul(
        left_imag, real_part, precision=exact_mode
    )
    return jnp.stack([rot_real, rot_imag])


def complex_table(table, count):
    cosine, sine_table = table
    real_rows = jnp.stack([cosine, sine_table], axis=1)
    imag_rows = jnp.stack([-sine_table, cosine], axis=1)
    scale = count.astype(jnp.float32)[None, :, None, None]
    return jnp.stack([real_rows, imag_rows]) / scale


def local_general(bloch_elements, gauge, kq_index, qpoint, re_vectors, re_weight, rp_vectors, rp_weight):
    local_k = bloch_elements.shape[1]
    local_q = bloch_elements.shape[2]
    bands = bloch_elements.shape[3]
    pairs = bands * bands
    gathered = lax.all_gather(gauge, "ka", axis=1, tiled=True)
    left_side = jnp.take(gathered, kq_index, axis=1)
    rotated = rotate_gauge(bloch_elements, left_side, gauge[:, :, None])
    rotated = rotated.reshape(2, local_k, local_q, pairs)
    k_count = gathered.shape[1]
    q_count = qpoint.shape[0]
    k_table = mesh_phase(re_vectors, jnp.arange(k_count, dtype=jnp.int32), k_count)
    q_table = mesh_phase(rp_vectors, qpoint, q_count)
    ka_count = lax.axis_size("ka")
    pb_count = lax.axis_size("pb")
    re_local = re_vectors.shape[0] // ka_count
    rp_local = rp_vectors.shape[0] // pb_count
    devices = ka_count * pb_count
    column_width = pairs // devices
    leaving = rotated.reshape(2, local_k, local_q, devices, column_width).transpose(3, 0, 1, 2, 4)
    leaving = leaving.reshape(devices, 2 * local_k * local_q, column_width)
    joined = lax.all_to_all(leaving, ("ka", "pb"), split_axis=0, concat_axis=0, tiled=True)
    joined = joined.reshape(ka_count, pb_count, 2, local_k, local_q, column_width)
    k_blocks = complex_table(k_table, re_weight).reshape(
        2, ka_count, re_local, 2, ka_count, local_k
    )
    q_blocks = complex_table(q_table, rp_weight).reshape(
        2, pb_count, rp_local, 2, pb_count, local_q
    )
    exact_mode = lax.Precision.HIGH
    electron = jnp.einsum("dauemk,mpeklx->dauplx", k_blocks, joined, precision=exact_mode)
    spread = jnp.einsum("fbvdpl,dauplx->abfuvx", q_blocks, electron, precision=exact_mode)
    spread = spread.reshape(devices, 2 * re_local * rp_local, column_width)
    result = lax.all_to_all(spread, ("ka", "pb"), split_axis=0, concat_axis=0, tiled=True)
    result = result.reshape(devices, 2, re_local, rp_local, column_width)
    return result.transpose(1, 2, 3, 0, 4).reshape(2, re_local, rp_local, bands, bands)


def split(x):
    high = x.astype(jnp.bfloat16)
    low = (x - high.astype(jnp.float32)).astype(jnp.bfloat16)
    return high, low


def dot(a, b):
    return jnp.dot(a, b, preferred_element_type=jnp.float32)


def swap(x, sign):
    return pltpu.roll(x, x.shape[-1] // 2, x.ndim - 1) * sign


class Plan:
    def __init__(self, ka, pb, local_k, local_q, bands, re_count, rp_count):
        self.ka, self.pb, self.half = ka, pb, pb // 2
        self.devices = ka * pb
        self.local_k, self.local_q, self.bands = local_k, local_q, bands
        self.k_count, self.q_count = ka * local_k, pb * local_q
        self.re_count, self.rp_count = re_count, rp_count
        self.re_local, self.rp_local = re_count // ka, rp_count // pb
        self.fits = (
            2 * bands == LANES
            and bands % self.devices == 0
            and pb & (pb - 1) == 0
            and pb > 2
            and ka % 2 == 0
            and local_k % 6 == 0
        )
        if not self.fits:
            return
        self.kb = local_k // 3
        self.kn = local_k - self.kb
        self.rows = bands // self.devices
        self.share = self.rows * local_q
        self.wide = 2 * self.share
        self.width = self.rows * pb
        self.piece = ka * self.kn
        self.chunks = self.rp_local * self.rows
        self.sources = pb + self.half
        self.block = self.re_local * pb
        self.raw_ahead = min(3, self.kb)
        self.g_slots = 3
        self.slots = 2
        self.ahead = 4
        self.fits = (
            self.share % 8 == 0
            and self.k_count % 16 == 0
            and self.kb % 2 == 0
            and (ka * self.kb) % 8 == 0
            and (pb * self.share) % 16 == 0
            and pb % 8 == 0
            and self.chunks > self.slots
            and self.rp_local > UNPACK_SLOTS
        )


def digits(point):
    return point // (MK2 * MK3), point // MK3 % MK2, point % MK3


def phases(columns, points, count):
    first, second, third = (d.astype(jnp.float32) for d in digits(points))
    total = MK1 * MK2 * MK3
    turns = (
        columns[:, 0:1] * (first * (MK2 * MK3))
        + columns[:, 1:2] * (second * (MK1 * MK3))
        + columns[:, 2:3] * (third * (MK1 * MK2))
    )
    turns = turns - total * jnp.floor((turns + 0.5) / total)
    angles = turns * (2.0 * math.pi / total)
    weight = columns[:, 3:4]
    return jnp.cos(angles) / count / weight, jnp.sin(angles) / count / weight


def pick(rows, values):
    source = lax.broadcasted_iota(jnp.int32, (rows.shape[0], values.shape[1]), 1)
    chosen = jnp.where(rows == source, 1.0, 0.0).astype(jnp.bfloat16)
    return lax.dot_general(
        chosen,
        values.astype(jnp.bfloat16),
        (((1,), (1,)), ((), ())),
        preferred_element_type=jnp.float32,
    )


def put_table(table, real, imag):
    full = jnp.concatenate([real, imag], axis=0)
    high, low = split(full)
    high = high.astype(jnp.float32)
    full = jnp.concatenate([high, low.astype(jnp.float32), high], axis=1)
    table[...] = full.astype(jnp.bfloat16)


def make_tables(p, side, slots, re, rp, tq, tf, tk):
    f32 = jnp.float32
    iota = lambda shape, dim: lax.broadcasted_iota(jnp.int32, shape, dim)
    re, rp = re.astype(f32), rp.astype(f32)

    def q_table(table, start, count, rows, inner):
        row = iota((count * rows, 1), 0)
        band = row % rows % inner * (rows // inner) + row % rows // inner
        columns = pick(start + row // rows, rp)
        width = rows * p.q_count
        col = iota((1, width), 1)
        slot = col // (rows * p.local_q) * p.local_q + col % p.local_q
        chosen = jnp.where(iota((p.q_count, width), 0) == slot, 1.0, 0.0)
        held = jnp.broadcast_to(slots[...], (8, p.q_count)).astype(f32)
        points = dot(held.astype(jnp.bfloat16), chosen.astype(jnp.bfloat16))[0:1]
        cosine, sine = phases(columns, points.astype(jnp.int32), p.q_count)
        same = band == col // p.local_q % rows
        put_table(table, jnp.where(same, cosine, 0.0), jnp.where(same, sine, 0.0))

    q_table(tq, 0, p.rp_count, p.rows, 1)
    q_table(tf, side * (p.rp_count // 2), p.rp_count // 2, 2 * p.rows, 2)

    columns = pick(iota((p.re_count, 1), 0), re)
    col = iota((1, p.k_count), 1)
    near = p.ka * p.kn
    point = jnp.where(
        col < near,
        col // p.kn * p.local_k + p.kb + col % p.kn,
        (col - near) // p.kb * p.local_k + (col - near) % p.kb,
    )
    cosine, sine = phases(columns, point, p.k_count)
    put_table(tk, cosine, sine)


def kernel(
    p,
    bloch,
    gauge_in,
    qpoint,
    slots,
    re_vectors,
    re_weight,
    rp_vectors,
    rp_weight,
    out,
    tq,
    tf,
    tk,
    gauge,
    gbuf,
    vg,
    rot,
    far,
    x_buf,
    xf_buf,
    y_buf,
    z_buf,
    w_buf,
    g_sem,
    u_sem,
    vs_sem,
    v1_sem,
    f_sem,
    v2_sem,
    s0_sem,
    r0_sem,
    s1_sem,
    r1_sem,
    sf_sem,
    rf_sem,
    s2_sem,
    r2_sem,
    s3_sem,
    r3_sem,
):
    a = lax.axis_index("ka")
    b = lax.axis_index("pb")
    core = b % 2
    sibling = b + 1 - 2 * core
    side = b // p.half
    seat = b % p.half
    other = seat + (1 - side) * p.half
    middle = p.local_k // 2
    lane = lax.broadcasted_iota(jnp.int32, (1, LANES), 1)
    sign = jnp.where(lane < p.bands, 1.0, -1.0).astype(jnp.float32)

    def xor(x, o, count):
        t, bit = 0, 1
        while bit < count:
            t = t + (x // bit + o // bit) % 2 * bit
            bit *= 2
        return t

    def load_g(k):
        slot = k % p.g_slots
        return pltpu.make_async_copy(bloch.at[:, k], gbuf.at[slot], g_sem.at[slot])

    load_u = pltpu.make_async_copy(gauge_in, gauge, u_sem)
    load_u.start()
    for k in range(p.g_slots):
        load_g(k).start()

    barrier = pltpu.get_barrier_semaphore()
    me = a * p.pb + b

    @pl.loop(1, p.devices)
    def _(o):
        t = (me + o) % p.devices
        pl.semaphore_signal(barrier, inc=1, device_id=(t // p.pb, t % p.pb), device_id_type=MESH)

    load_u.wait()

    @pl.loop(0, p.local_k)
    def _(k):
        v = jnp.concatenate([jnp.transpose(gauge[0, k]), jnp.transpose(gauge[1, k])], axis=1)
        for t in range(p.ka):
            for r in range(p.rows):
                first = t * p.width + r * p.pb
                where = pl.ds(t * p.width + r, p.pb, stride=p.rows)
                vg[a * p.local_k + k, where, :] = v[first : first + p.pb]

    pl.semaphore_wait(barrier, p.devices - 1)

    def send_v(i):
        return pltpu.make_async_remote_copy(
            src_ref=vg.at[pl.ds(a * p.local_k + core * middle, middle)],
            dst_ref=vg.at[pl.ds(a * p.local_k + core * middle, middle)],
            send_sem=vs_sem.at[i],
            recv_sem=v1_sem.at[i],
            device_id=((a + i) % p.ka, b),
            device_id_type=MESH,
        )

    def pass_v(i):
        source = (a + p.ka - i) % p.ka
        part = pl.ds(source * p.local_k + core * middle, middle)
        return pltpu.make_async_remote_copy(
            src_ref=vg.at[part],
            dst_ref=vg.at[part],
            send_sem=f_sem.at[i],
            recv_sem=v2_sem.at[i],
            device_id=(a, sibling),
            device_id_type=MESH,
        )

    for i in range(1, p.ka):
        send_v(i).start()

    def right_side(k, carry):
        load_g(k).wait()
        g = gbuf[k % p.g_slots]
        g = jnp.concatenate([g[0], g[1]], axis=-1).reshape(p.local_q * p.bands, LANES)
        g_high, g_low = split(g)
        u, v = gauge[0, k], gauge[1, k]
        r_high, r_low = split(
            jnp.concatenate(
                [jnp.concatenate([u, v], axis=1), jnp.concatenate([-v, u], axis=1)], axis=0
            )
        )
        h = dot(
            jnp.concatenate([g_high, g_low], axis=1), jnp.concatenate([r_high, r_high], axis=0)
        ) + dot(g_high, r_low)
        h = h.reshape(p.local_q, p.bands, LANES)
        for q in range(p.local_q):
            rot[k, pl.ds(q, p.bands, stride=p.local_q), :] = h[q]

        @pl.when(k + p.g_slots < p.local_k)
        def _():
            load_g(k + p.g_slots).start()

        return carry

    def send_0(k):
        return pltpu.make_async_remote_copy(
            src_ref=rot.at[k],
            dst_ref=far.at[k],
            send_sem=s0_sem.at[k],
            recv_sem=r0_sem.at[k],
            device_id=(a, other),
            device_id_type=MESH,
        )

    @pl.loop(0, p.raw_ahead)
    def _(k):
        right_side(k, 0)
        send_0(k).start()

    lax.fori_loop(p.raw_ahead, middle, right_side, 0)
    re = jnp.concatenate([re_vectors[...], re_weight[...]], axis=0)
    rp = jnp.concatenate([rp_vectors[...], rp_weight[...]], axis=0)
    make_tables(p, side, slots, re, rp, tq, tf, tk)
    for i in range(1, p.ka):
        send_v(i).wait_recv()
        pass_v(i).start()
    lax.fori_loop(middle, p.local_k, right_side, 0)
    for i in range(1, p.ka):
        pass_v(i).wait_recv()

    def left_side(buf, row, k, source):
        k1, k2, k3 = digits(a * p.local_k + k)
        for q in range(p.local_q):
            q1, q2, q3 = digits(qpoint[source * p.local_q + q])
            kq = ((k1 + q1) % MK1 * MK2 + (k2 + q2) % MK2) * MK3 + (k3 + q3) % MK3
            v_high, v_low = split(vg[kq])
            h = buf[row, pl.ds(q, p.bands, stride=p.local_q), :]
            h_high, h_low = split(jnp.concatenate([h, swap(h, sign)], axis=0))
            buf[row, pl.ds(q, p.bands, stride=p.local_q), :] = dot(
                jnp.concatenate([v_high, v_low], axis=1),
                jnp.concatenate([h_high, h_high], axis=0),
            ) + dot(v_high, h_low)

    def send_1(c, n):
        ta = (a + p.ka - 1 - n % p.ka) % p.ka
        tb = xor(b, p.pb - 1 - n // p.ka, p.pb)
        t = ta * p.pb + tb
        return pltpu.make_async_remote_copy(
            src_ref=rot.at[p.kb + c, pl.ds(t * p.share, p.share)],
            dst_ref=x_buf.at[a, c, b],
            send_sem=s1_sem.at[c],
            recv_sem=r1_sem.at[c],
            device_id=(ta, tb),
            device_id_type=MESH,
        )

    def own_1(c):
        return pltpu.make_async_copy(
            rot.at[p.kb + c, pl.ds(me * p.share, p.share)], x_buf.at[a, c, b], r1_sem.at[c]
        )

    def send_f(buf, k, came_from, n):
        ta = (a + p.ka - 1 - n % p.ka) % p.ka
        ts = xor(seat, p.half - 1 - n // p.ka, p.half)
        t = ta * p.half + ts
        return pltpu.make_async_remote_copy(
            src_ref=buf.at[k, pl.ds(t * p.wide, p.wide)],
            dst_ref=xf_buf.at[a, k, came_from],
            send_sem=sf_sem.at[k],
            recv_sem=rf_sem.at[k],
            device_id=(ta, side * p.half + ts),
            device_id_type=MESH,
        )

    def own_f(buf, k, came_from):
        t = a * p.half + seat
        return pltpu.make_async_copy(
            buf.at[k, pl.ds(t * p.wide, p.wide)], xf_buf.at[a, k, came_from], rf_sem.at[k]
        )

    def add_q(table, x, first, rows, stride, gap):
        x_high, x_low = split(x)
        y = dot(table[...], jnp.concatenate([x_high, x_high, x_low], axis=0))
        for j in range(2):
            cols = slice(j * LANES, (j + 1) * LANES)
            where = pl.ds(first + j * gap, rows, stride=stride)
            y_buf[where, :] = y[:rows, cols] + swap(y[rows:, cols], sign)

    far_first = p.pb * p.chunks * p.piece

    def sum_near(c):
        part = x_buf.at[:, pl.ds(c, 1)]
        pltpu.make_async_copy(part, part, r1_sem.at[c]).wait()

        @pl.loop(0, p.ka // 2)
        def _(pair):
            x = jnp.concatenate(
                [
                    x_buf[2 * pair, c].reshape(p.pb * p.share, LANES),
                    x_buf[2 * pair + 1, c].reshape(p.pb * p.share, LANES),
                ],
                axis=1,
            )
            add_q(tq, x, 2 * pair * p.kn + c, p.rp_count * p.rows, p.ka * p.kn, p.kn)

    def sum_far(c):
        part = xf_buf.at[:, pl.ds(c, 1)]
        pltpu.make_async_copy(part, part, rf_sem.at[c]).wait()

        @pl.loop(0, p.ka // 2)
        def _(pair):
            x = jnp.concatenate(
                [
                    xf_buf[2 * pair, c].reshape(p.pb * p.wide, LANES),
                    xf_buf[2 * pair + 1, c].reshape(p.pb * p.wide, LANES),
                ],
                axis=1,
            )
            add_q(
                tf,
                x,
                far_first + 2 * pair * p.kb + c,
                p.rp_count * p.rows,
                p.ka * p.kb,
                p.kb,
            )

    def begin(c):
        return c * c * p.kn // (p.kb * p.kb)

    def stay(c):
        @pl.loop(begin(c), begin(c + 1))
        def _(k):
            left_side(rot, p.kb + k, p.kb + k, b)

            @pl.loop(0, p.devices - 1)
            def _(n):
                send_1(k, n).start()

            own_1(k).start()

    def swapped(c):
        send_0(c).wait_send()
        left_side(rot, c, c, b)

        @pl.loop(0, p.ka * p.half - 1)
        def _(n):
            send_f(rot, c, b, n).start()

        own_f(rot, c, b).start()
        send_0(c).wait_recv()
        left_side(far, c, c, other)

        @pl.loop(0, p.ka * p.half - 1)
        def _(n):
            send_f(far, c, other, n).start()

        own_f(far, c, other).start()

    @pl.loop(0, p.kb + 2)
    def _(c):
        @pl.when(c < p.kb)
        def _():
            @pl.loop(0, 2)
            def _(turn):
                @pl.when(turn == core)
                def _():
                    swapped(c)

                @pl.when(turn != core)
                def _():
                    stay(c)

            @pl.when(c + p.raw_ahead < p.kb)
            def _():
                send_0(c + p.raw_ahead).start()

        @pl.when(c >= 2)
        def _():
            sum_far(c - 2)
            pl.loop(begin(c - 2), begin(c - 2 + 1))(sum_near)

    def send_2(j, o):
        t = xor(b, o, p.pb)
        return pltpu.make_async_remote_copy(
            src_ref=y_buf.at[pl.ds((t * p.chunks + j) * p.piece, p.piece)],
            dst_ref=z_buf.at[j, b],
            send_sem=s2_sem.at[j],
            recv_sem=r2_sem.at[j],
            device_id=(a, t),
            device_id_type=MESH,
        )

    def send_2f(j, o):
        t = xor(seat, o, p.half)
        return pltpu.make_async_remote_copy(
            src_ref=y_buf.at[pl.ds(((p.pb + t) * p.chunks + j) * p.piece, p.piece)],
            dst_ref=z_buf.at[j, p.pb + seat],
            send_sem=s2_sem.at[j],
            recv_sem=r2_sem.at[j],
            device_id=(a, side * p.half + t),
            device_id_type=MESH,
        )

    def start_2(j):
        @pl.loop(1, p.pb)
        def _(o):
            send_2(j, o).start()

        @pl.loop(1, p.half)
        def _(o):
            send_2f(j, o).start()

        for mine in (b, p.pb + seat):
            pltpu.make_async_copy(
                y_buf.at[pl.ds((mine * p.chunks + j) * p.piece, p.piece)],
                z_buf.at[j, mine],
                r2_sem.at[j],
            ).start()

    for j in range(p.ahead):
        start_2(j)

    def send_3(j, o):
        t = (a + o) % p.ka
        slot = j % p.slots
        return pltpu.make_async_remote_copy(
            src_ref=w_buf.at[slot, t],
            dst_ref=out.at[j, a],
            send_sem=s3_sem.at[slot],
            recv_sem=r3_sem.at[j],
            device_id=(t, b),
            device_id_type=MESH,
        )

    def own_3(j):
        slot = j % p.slots
        return pltpu.make_async_copy(w_buf.at[slot, a], out.at[j, a], g_sem.at[slot])

    def free_3(j):
        slot = j % p.slots
        sent = w_buf.at[slot, pl.ds(0, p.ka - 1)]
        pltpu.make_async_copy(sent, sent, s3_sem.at[slot]).wait()
        own_3(j).wait()

    less = p.ka * p.kb

    @pl.loop(0, p.chunks)
    def _(j):
        pltpu.make_async_copy(z_buf.at[j], z_buf.at[j], r2_sem.at[j]).wait()
        slot = j % p.slots

        @pl.when(j + p.ahead < p.chunks)
        def _():
            start_2(j + p.ahead)

        @pl.when(j >= p.slots)
        def _():
            free_3(j - p.slots)

        @pl.loop(0, p.half)
        def _(s):
            far_part = z_buf[j, p.pb + s]
            z = jnp.concatenate(
                [
                    jnp.concatenate(
                        [z_buf[j, 2 * s + i], far_part[i * less : (i + 1) * less]], axis=0
                    )
                    for i in range(2)
                ],
                axis=1,
            )
            z_high, z_low = split(z)
            w = dot(tk[...], jnp.concatenate([z_high, z_high, z_low], axis=0))
            for i in range(2):
                cols = slice(i * LANES, (i + 1) * LANES)
                full = w[: p.re_count, cols] + swap(w[p.re_count :, cols], sign)
                where = pl.ds(2 * s + i, p.re_local, stride=p.pb)
                for t in range(p.ka):
                    w_buf[slot, t, where, :] = full[t * p.re_local : (t + 1) * p.re_local]

        @pl.loop(1, p.ka)
        def _(o):
            send_3(j, o).start()

        own_3(j).start()

    for j in range(p.chunks - p.slots, p.chunks):
        free_3(j)

    @pl.loop(0, p.chunks)
    def _(j):
        into = out.at[j, pl.ds(0, p.ka - 1)]
        pltpu.make_async_copy(into, into, r3_sem.at[j]).wait()
        sent = z_buf.at[j, pl.ds(0, p.sources - 2)]
        pltpu.make_async_copy(sent, sent, s2_sem.at[j]).wait()

    @pl.loop(0, p.kn)
    def _(c):
        sent = rot.at[c, pl.ds(0, (p.devices - 1) * p.share)]
        pltpu.make_async_copy(sent, sent, s1_sem.at[c]).wait()

    @pl.loop(0, p.kb)
    def _(c):
        sent = rot.at[pl.ds(c, 2), pl.ds(0, (p.ka * p.half - 1) * p.wide)]
        pltpu.make_async_copy(sent, sent, sf_sem.at[c]).wait()

    for i in range(1, p.ka):
        send_v(i).wait_send()
        pass_v(i).wait_send()


def unpack(p, x_ref, o_ref, x_buf, o_buf, x_sem, o_sem):
    def load(j):
        slot = j % UNPACK_SLOTS
        return pltpu.make_async_copy(
            x_ref.at[pl.ds(j * p.rows, p.rows)], x_buf.at[slot], x_sem.at[slot]
        )

    def store(j):
        slot = j % UNPACK_SLOTS
        return pltpu.make_async_copy(o_buf.at[slot], o_ref.at[:, :, j], o_sem.at[slot])

    for j in range(UNPACK_SLOTS):
        load(j).start()

    @pl.loop(0, p.rp_local)
    def _(j):
        slot = j % UNPACK_SLOTS
        load(j).wait()

        @pl.when(j >= UNPACK_SLOTS)
        def _():
            store(j - UNPACK_SLOTS).wait()

        for r in range(p.rows):
            for t in range(p.ka):
                x = x_buf[slot, r, t].reshape(p.re_local, p.pb, LANES)
                first = t * p.width + r * p.pb
                o_buf[slot, 0, :, first : first + p.pb, :] = x[..., : p.bands]
                o_buf[slot, 1, :, first : first + p.pb, :] = x[..., p.bands :]
        store(j).start()

        @pl.when(j + UNPACK_SLOTS < p.rp_local)
        def _():
            load(j + UNPACK_SLOTS).start()

    for j in range(p.rp_local - UNPACK_SLOTS, p.rp_local):
        store(j).wait()


def local_fused(p, bloch, gauge, _, qpoint, re_vectors, re_weight, rp_vectors, rp_weight):
    rows_q = 2 * p.rp_count * p.rows
    f32 = jnp.float32
    dma = pltpu.SemaphoreType.DMA
    vmem = pl.BlockSpec(memory_space=pltpu.VMEM)
    any_space = pl.BlockSpec(memory_space=pl.ANY)
    smem = pl.BlockSpec(memory_space=pltpu.SMEM)
    landed = pl.pallas_call(
        functools.partial(kernel, p),
        out_shape=jax.ShapeDtypeStruct((p.chunks, p.ka, p.block, LANES), f32),
        in_specs=[any_space, any_space, smem, vmem, vmem, vmem, vmem, vmem],
        out_specs=any_space,
        scratch_shapes=[
            pltpu.VMEM((rows_q, 3 * p.rows * p.q_count), jnp.bfloat16),
            pltpu.VMEM((rows_q, 6 * p.rows * p.q_count), jnp.bfloat16),
            pltpu.VMEM((2 * p.re_count, 3 * p.k_count), jnp.bfloat16),
            pltpu.VMEM((2, p.local_k, p.bands, p.bands), f32),
            pltpu.VMEM((p.g_slots, 2, p.local_q, p.bands, p.bands), f32),
            pltpu.VMEM((p.k_count, p.bands, LANES), f32),
            pltpu.VMEM((p.local_k, p.devices * p.share, LANES), f32),
            pltpu.VMEM((p.kb, p.devices * p.share, LANES), f32),
            pltpu.VMEM((p.ka, p.kn, p.pb, p.share, LANES), f32),
            pltpu.VMEM((p.ka, p.kb, p.pb, p.wide, LANES), f32),
            pltpu.VMEM((p.sources * p.chunks * p.piece, LANES), f32),
            pltpu.VMEM((p.chunks, p.sources, p.piece, LANES), f32),
            pltpu.VMEM((p.slots, p.ka, p.block, LANES), f32),
            dma((max(p.g_slots, p.slots),)),
            dma,
            dma((p.ka,)),
            dma((p.ka,)),
            dma((p.ka,)),
            dma((p.ka,)),
            dma((p.kb,)),
            dma((p.kb,)),
            dma((p.kn,)),
            dma((p.kn,)),
            dma((p.kb,)),
            dma((p.kb,)),
            dma((p.chunks,)),
            dma((p.chunks,)),
            dma((p.slots,)),
            dma((p.chunks,)),
        ],
        compiler_params=pltpu.CompilerParams(
            collective_id=0, has_side_effects=True, vmem_limit_bytes=VMEM_BYTES
        ),
    )(
        bloch,
        gauge,
        qpoint,
        qpoint.reshape(1, -1),
        re_vectors.T,
        re_weight.reshape(1, -1),
        rp_vectors.T,
        rp_weight.reshape(1, -1),
    )

    return pl.pallas_call(
        functools.partial(unpack, p),
        out_shape=jax.ShapeDtypeStruct((2, p.re_local, p.rp_local, p.bands, p.bands), f32),
        in_specs=[any_space],
        out_specs=any_space,
        scratch_shapes=[
            pltpu.VMEM((UNPACK_SLOTS, p.rows, p.ka, p.block, LANES), f32),
            pltpu.VMEM((UNPACK_SLOTS, 2, p.re_local, p.bands, p.bands), f32),
            dma((UNPACK_SLOTS,)),
            dma((UNPACK_SLOTS,)),
        ],
        compiler_params=pltpu.CompilerParams(vmem_limit_bytes=VMEM_BYTES),
    )(landed)


def local(bloch_elements, gauge, kq_index, qpoint, re_vectors, re_weight, rp_vectors, rp_weight):
    p = Plan(
        lax.axis_size("ka"),
        lax.axis_size("pb"),
        bloch_elements.shape[1],
        bloch_elements.shape[2],
        bloch_elements.shape[3],
        re_vectors.shape[0],
        rp_vectors.shape[0],
    )
    program = functools.partial(local_fused, p) if p.fits else local_general
    return program(
        bloch_elements, gauge, kq_index, qpoint, re_vectors, re_weight, rp_vectors, rp_weight
    )


def solution(mesh):
    placed = (
        P(None, "ka", "pb", None, None),
        P(None, "ka", None, None),
        P("ka", "pb"),
        P(),
        P(),
        P(),
        P(),
        P(),
    )
    return jax.shard_map(
        local,
        mesh=mesh,
        in_specs=placed,
        out_specs=P(None, "ka", "pb", None, None),
        check_vma=False,
    )
```
